128 devices in a mesh: tok: 8 (over z_lo, x), row: 4 (over z_hi, core), col: 4 (over y).
Axes of the slice: x: 4, y: 4, z: 4 (z_hi: 2, z_lo: 2; z = z_hi * 2 + z_lo), core: 2. Of those that a mesh axis runs over, the one named last changes fastest.
Arguments:
- activations: bfloat16 [2, 1024, 28672], P(None, 'tok', ('row', 'col')), may hold values from -0.1875 to 0.1875
- weights: bfloat16 [2, 28672, 8192], P(None, ('row', 'col'), 'tok'), may hold values from -6 to 6
Outputs:
- solved: float32 [256, 8192], P('row', ('tok', 'col'))
- correction: bfloat16 [28672, 8192], P(('row', 'col'), 'tok')
The draws below stay inside these ranges and needn't reach their ends.
All inputs are finite; a program needn't handle non-finite values.
Results may differ from the reference program's by a relative error of at most 0.0073.
Values may be sent and summed in bfloat16 or wider, within the bound.
A program may use at most 64 MiB of HBM per device.

```python
import jax
import jax.numpy as jnp
from jax import lax

IN = 28672
OUT = 8192
PANEL = 256
TOKENS = 1024


def block_scale(stream_key, extent, shards, least, high):
    loudness = 1.0
    for axis_at, blocks in shards:
        heights = jax.random.uniform(jax.random.fold_in(jax.random.fold_in(stream_key, 6), axis_at), (blocks,), jnp.float32, least / len(shards), high / len(shards))
        loudness = loudness * jnp.repeat(jnp.exp(heights), extent[axis_at] // blocks).reshape((-1,) + (1,) * (len(extent) - 1 - axis_at))
    return loudness


def centred(own_key, extent, scale, most, pieces=(), kind=jnp.bfloat16):
    array = scale * jax.random.normal(own_key, extent, jnp.float32)
    if pieces:
        array = array * block_scale(own_key, extent, pieces, -0.22, 0.18)
    return jnp.clip(array, -most, most).astype(kind)


def setup_inputs(seed: int = 0) -> dict:
    keys = jax.random.split(jax.random.key(seed), 3)
    activations = centred(keys[0], (2, TOKENS, IN), (TOKENS ** -0.5), 0.1875, ((1, 8), (2, 16)))
    weights = centred(keys[1], (2, IN, OUT), 1.0, 6.0, ((1, 16), (2, 8)))
    return {"activations": activations, "weights": weights}


def reference(activations, weights):
    panel_tokens = activations[:, :, :PANEL]
    grams = jnp.einsum('mti,mtp->mip', activations.astype(jnp.float32), panel_tokens.astype(jnp.float32), precision=lax.Precision.HIGHEST)
    row_ids = jnp.arange(IN, dtype=jnp.int32)[:, None]
    col_ids = jnp.arange(PANEL, dtype=jnp.int32)[None, :]
    on_diagonal = row_ids == col_ids
    regular = grams * jnp.where(on_diagonal, 1.0, 0.9).astype(jnp.float32)[None]
    regular_bf16 = regular.astype(jnp.bfloat16)
    summed = regular[0] + regular[1]
    right_side = jnp.dot(regular_bf16[0].T.astype(jnp.float32), weights[0].astype(jnp.float32), preferred_element_type=jnp.float32)
    right_side = right_side + jnp.dot(regular_bf16[1].T.astype(jnp.float32), weights[1].astype(jnp.float32), preferred_element_type=jnp.float32)
    factor = jnp.linalg.cholesky(summed[:PANEL])
    panel_factor = lax.linalg.triangular_solve(factor, summed, left_side=False, lower=True, transpose_a=True)
    solved = lax.linalg.triangular_solve(factor, right_side, left_side=True, lower=True)
    correction = jnp.dot(panel_factor.astype(jnp.float32), solved.astype(jnp.float32), precision=lax.Precision.HIGHEST, preferred_element_type=jnp.float32)
    return (solved, correction.astype(jnp.bfloat16))
```

```python
import jax
import jax.numpy as jnp
from jax import lax
from jax.experimental import pallas as pl
from jax.experimental.pallas import tpu as pltpu
from jax.sharding import PartitionSpec as P

PANEL = 256
STEP = 16
MESH = pl.DeviceIdType.MESH
HIGHEST = lax.Precision.HIGHEST
F32 = jnp.float32
BF16 = jnp.bfloat16


def split3(value):
    high = value.astype(BF16)
    rest = value - high.astype(F32)
    middle = rest.astype(BF16)
    low = (rest - middle.astype(F32)).astype(BF16)
    return high, middle, low


def eliminate(step, big):
    base = pl.multiple_of(step * STEP, STEP)
    per_half = 128 // STEP
    rows = [big[h, pl.ds(base, STEP), :] for h in range(4)]
    shift = lax.rem(128 - lax.rem(step, per_half) * STEP, 128)
    diag = pltpu.roll(big[step // per_half, pl.ds(base, STEP), :], shift, 1)
    cols = [jnp.broadcast_to(diag[:, j : j + 1], (STEP, 128)) for j in range(STEP)]
    ids = lax.broadcasted_iota(jnp.int32, (STEP, 128), 0)
    for p in range(STEP):
        inverse = lax.rsqrt(cols[p][p : p + 1, :])
        lcol = cols[p] * inverse
        below = jnp.where(ids > p, lcol, 0.0)
        for h in range(4):
            pivot = rows[h][p : p + 1, :] * inverse
            rows[h] = jnp.where(ids == p, pivot, rows[h] - below * pivot)
        for j in range(p + 1, STEP):
            cols[j] = cols[j] - lcol * lcol[j : j + 1, :]
    for h in range(4):
        big[h, pl.ds(base, STEP), :] = rows[h]
    wide = jnp.concatenate(rows, axis=1)
    lane = lax.broadcasted_iota(jnp.int32, (STEP, PANEL), 1)
    left = jnp.where(lane >= base + STEP, wide[:, :PANEL], 0.0)
    lh, lm, ll = split3(left)
    rh, rm, rl = split3(wide)
    lhs = jnp.concatenate([lh, lh, lm, lm, lh, ll], axis=0)
    rhs = jnp.concatenate([rh, rm, rh, rm, rl, rh], axis=0)
    update = lax.dot_general(
        lhs, rhs, (((0,), (0,)), ((), ())), preferred_element_type=F32
    )
    for h in range(4):
        big[h] = big[h] - update[:, 128 * h : 128 * h + 128]


def first_unit(t, core):
    return 7 * (t // 2) + lax.rem(t, 2) * (4 - core)


def has_fourth(t, core):
    return lax.rem(t + core, 2) == 0


def kernel(
    acts, wts, zout, smout, solout,
    xv, wv, pb, pt, xg, gt, rp, rsend, rin, r2, r2in, zb, solb, solin, big, sinv,
    xsem, wsem, p1send, p2send, p3send, precv, xsend, xrecv, gsend, grecv,
    dsend, drecv, rsems, rrecv, zsend, zfwd, zrecv, ssend, srecv,
):
    t = lax.axis_index("tok")
    row = lax.axis_index("row")
    col = lax.axis_index("col")
    core = lax.rem(row, 2)
    zhi = row // 2
    partner = {"row": row + 1 - 2 * core}

    def remote(src, dst, ss, rs, dev):
        return pltpu.make_async_remote_copy(
            src_ref=src, dst_ref=dst, send_sem=ss, recv_sem=rs, device_id=dev,
            device_id_type=MESH,
        )

    def arrived(ref, sem):
        pltpu.make_async_copy(ref, ref, sem).wait()

    load_x = pltpu.make_async_copy(acts, xv, xsem)
    load_x.start()
    load_w = pltpu.make_async_copy(wts, wv, wsem)
    load_w.start()

    barrier = pltpu.get_barrier_semaphore()
    for d in range(1, 8):
        pl.semaphore_signal(
            barrier, inc=1, device_id={"tok": lax.rem(t + d, 8)}, device_id_type=MESH
        )
    for e in range(1, 16):
        dev = {"row": lax.rem(row + e // 4, 4), "col": lax.rem(col + e % 4, 4)}
        pl.semaphore_signal(barrier, inc=1, device_id=dev, device_id_type=MESH)
    load_x.wait()
    pl.semaphore_wait(barrier, 22)

    source = jnp.logical_and(row == 0, col == 0)

    def p1(e):
        m = (e // 4) % 2
        return remote(
            xv.at[m, :, 0:PANEL], pb.at[m, t], p1send.at[e], precv.at[m, t],
            {"row": e // 4, "col": e % 4},
        )

    @pl.when(source)
    def _():
        pltpu.make_async_copy(acts.at[0, :, 0:PANEL], pb.at[0, t], precv.at[0, t]).start()
        for e in range(1, 16):
            p1(e).start()

    def xcopy(d, slot):
        tt = lax.rem(t + d, 8)
        unit = first_unit(tt, core) + slot
        lanes = pl.ds(pl.multiple_of(lax.rem(unit, 14) * 128, 128), 128)
        if d == 0:
            return pltpu.make_async_copy(
                acts.at[unit // 14, :, lanes], xg.at[slot, t], xrecv.at[slot]
            )
        return remote(
            xv.at[unit // 14, :, lanes], xg.at[slot, t], xsend.at[slot * 8 + d],
            xrecv.at[slot], {"tok": tt},
        )

    def send_slot(slot):
        for d in range(8):
            if slot < 3:
                xcopy(d, slot).start()
            else:
                @pl.when(has_fourth(lax.rem(t + d, 8), core))
                def _():
                    xcopy(d, slot).start()

    send_slot(0)

    def p2(d):
        return remote(
            pb.at[core, t], pb.at[core, t], p2send.at[d], precv.at[core, t],
            {"tok": lax.rem(t + d, 8)},
        )

    def p3(d):
        tt = lax.rem(t + d, 8)
        return remote(
            pb.at[core, tt], pb.at[core, tt], p3send.at[d], precv.at[core, tt], partner
        )

    arrived(pb.at[core, t], precv.at[core, t])
    for d in range(1, 8):
        p2(d).start()
    p3(0).start()
    for slot in range(1, 4):
        send_slot(slot)
    for d in range(1, 8):
        tt = lax.rem(t + d, 8)
        arrived(pb.at[core, tt], precv.at[core, tt])
        p3(d).start()
    for d in range(8):
        tt = lax.rem(t + d, 8)
        arrived(pb.at[1 - core, tt], precv.at[1 - core, tt])

    total = jnp.zeros((PANEL, PANEL), F32)
    for m in range(2):
        tokens = pb[m].reshape(1024, PANEL)
        flipped = jnp.transpose(tokens)
        pt[m] = flipped
        total = total + jnp.dot(flipped, tokens, preferred_element_type=F32)
    ii = lax.broadcasted_iota(jnp.int32, (PANEL, 128), 0)
    jj = lax.broadcasted_iota(jnp.int32, (PANEL, 128), 1)
    for h in range(2):
        on = ii == jj + 128 * h
        big[h] = total[:, 128 * h : 128 * h + 128] * jnp.where(on, 1.0, 0.9)
        big[2 + h] = jnp.where(on, 1.0, 0.0)

    def panels(first, last):
        def one(step, carry):
            eliminate(step, big)
            return carry

        lax.fori_loop(first, last, one, 0)

    panels(0, 5)

    own = first_unit(t, core)

    def gcopy(slot, d):
        return remote(
            gt.at[own + slot], gt.at[own + slot], gsend.at[slot * 8 + d],
            grecv.at[own + slot], {"tok": lax.rem(t + d, 8)},
        )

    def gram(slot):
        arrived(xg.at[slot], xrecv.at[slot])
        unit = own + slot
        first = (row * 4 + col) * 1792 + lax.rem(unit, 14) * 128
        product = jnp.dot(
            pt[unit // 14], xg[slot].reshape(1024, 128), preferred_element_type=F32
        )
        gt[unit] = (product * jnp.where(ii == jj + first, 1.0, 0.9)).astype(BF16)
        for d in range(1, 8):
            gcopy(slot, d).start()

    for slot in range(3):
        gram(slot)

    @pl.when(has_fourth(t, core))
    def _():
        gram(3)

    panels(5, 16)
    inverse = jnp.concatenate([big[2], big[3]], axis=1)
    sinv[...] = lax.dot_general(
        inverse, inverse, (((0,), (0,)), ((), ())), precision=HIGHEST,
        preferred_element_type=F32,
    )

    load_w.wait()
    count = jnp.where(has_fourth(t, core), 4, 3)

    def accumulate(i, carry):
        for k in range(2):
            unit = 2 * i + k

            @pl.when(jnp.logical_or(unit < own, unit >= own + count))
            def _():
                arrived(gt.at[unit], grecv.at[unit])

        lhs = jnp.concatenate([gt[2 * i], gt[2 * i + 1]], axis=1)
        feats = pl.ds(pl.multiple_of(lax.rem(i, 7) * 256, 256), 256)
        part = jnp.dot(lhs, wv[i // 7, feats, :], preferred_element_type=F32)
        for q in range(8):
            piece = part[:, 128 * q : 128 * q + 128]
            rp[q] = jnp.where(i == 0, piece, rp[q] + piece)
        return carry

    lax.fori_loop(0, 14, accumulate, 0)

    def flip(first, last):
        for j in range(first, last):
            both = gt[j].astype(F32) + gt[14 + j].astype(F32)
            smout[128 * j : 128 * j + 128, :] = jnp.transpose(both).astype(BF16)

    def group(i, which):
        return 2 * i + lax.rem(which + i, 2)

    def dcopy(i):
        return remote(rsend.at[i], rin.at[i], dsend.at[i], drecv.at[i], partner)

    for i in range(4):
        rsend[i] = rp[group(i, 1 - core)].astype(BF16)
        dcopy(i).start()
    flip(0, 5)
    solver = lax.rem(col + zhi, 2) == core
    chip = zhi * 4 + col
    mine = 2 * col + zhi

    def mine_is(i):
        return jnp.logical_and(solver, i == col)

    def rcopy(i):
        dev = {"row": 2 * lax.rem(core + i, 2) + core, "col": i}
        return remote(r2.at[i], r2in.at[chip], rsems.at[i], rrecv.at[chip], dev)

    for i in range(4):
        arrived(rin.at[i], drecv.at[i])
        r2[i] = (rp[group(i, core)] + rin[i].astype(F32)).astype(BF16)

        @pl.when(jnp.logical_not(mine_is(i)))
        def _():
            rcopy(i).start()

    flip(5, 10)

    def zcopy(e):
        dev = {
            "row": 2 * lax.rem(zhi + e // 4, 2) + core, "col": lax.rem(col + e % 4, 4)
        }
        return remote(zb.at[mine], zb.at[mine], zsend.at[e], zrecv.at[mine], dev)

    def scopy(rr):
        return remote(
            solb.at[pl.ds(64 * rr, 64), :], solin.at[zhi], ssend.at[rr], srecv.at[zhi],
            {"row": rr, "col": col},
        )

    @pl.when(solver)
    def _():
        whole = rp[mine] + rin[col].astype(F32)
        for e in range(1, 8):
            other = lax.rem(chip + e, 8)
            arrived(r2in.at[other], rrecv.at[other])
            whole = whole + r2in[other].astype(F32)
        answer = jnp.dot(sinv[...], whole, precision=HIGHEST, preferred_element_type=F32)
        zb[mine] = answer.astype(BF16)
        for e in range(1, 8):
            zcopy(e).start()
        inverse = jnp.concatenate([big[2], big[3]], axis=1)
        solb[...] = jnp.dot(inverse, whole, precision=HIGHEST, preferred_element_type=F32)
        for rr in range(4):
            @pl.when(rr != row)
            def _():
                scopy(rr).start()

            @pl.when(rr == row)
            def _():
                solin[zhi] = solb[64 * rr : 64 * rr + 64, :]

    flip(10, 14)

    def zforward(i):
        q = group(i, core)
        return remote(zb.at[q], zb.at[q], zfwd.at[i], zrecv.at[q], partner)

    for i in range(4):
        q = group(i, core)

        @pl.when(jnp.logical_not(mine_is(i)))
        def _():
            arrived(zb.at[q], zrecv.at[q])

        zforward(i).start()
    for i in range(4):
        q = group(i, 1 - core)
        arrived(zb.at[q], zrecv.at[q])
    for q in range(8):
        zout[:, 128 * q : 128 * q + 128] = zb[q]
    for h in range(2):
        @pl.when(jnp.logical_not(jnp.logical_and(solver, zhi == h)))
        def _():
            arrived(solin.at[h], srecv.at[h])

        solout[:, 128 * h : 128 * h + 128] = solin[h]

    @pl.when(source)
    def _():
        for e in range(1, 16):
            p1(e).wait_send()

    for d in range(8):
        p3(d).wait_send()
    for d in range(1, 8):
        p2(d).wait_send()
        for slot in range(3):
            xcopy(d, slot).wait_send()
            gcopy(slot, d).wait_send()

        @pl.when(has_fourth(lax.rem(t + d, 8), core))
        def _():
            xcopy(d, 3).wait_send()

        @pl.when(has_fourth(t, core))
        def _():
            gcopy(3, d).wait_send()

    for i in range(4):
        dcopy(i).wait_send()
        zforward(i).wait_send()

        @pl.when(jnp.logical_not(mine_is(i)))
        def _():
            rcopy(i).wait_send()

    @pl.when(solver)
    def _():
        for e in range(1, 8):
            zcopy(e).wait_send()
        for rr in range(4):
            @pl.when(rr != row)
            def _():
                scopy(rr).wait_send()


def body(activations, weights):
    dma = pltpu.SemaphoreType.DMA
    vmem = pltpu.VMEM
    outs = pl.pallas_call(
        kernel,
        out_shape=(
            jax.ShapeDtypeStruct((256, 1024), BF16),
            jax.ShapeDtypeStruct((1792, 256), BF16),
            jax.ShapeDtypeStruct((64, 256), F32),
        ),
        in_specs=[pl.BlockSpec(memory_space=pl.ANY)] * 2,
        out_specs=(pl.BlockSpec(memory_space=pltpu.VMEM),) * 3,
        scratch_shapes=[
            vmem((2, 128, 1792), BF16), vmem((2, 1792, 1024), BF16),
            vmem((2, 8, 128, 256), BF16), vmem((2, 256, 1024), BF16),
            vmem((4, 8, 128, 128), BF16), vmem((28, 256, 128), BF16),
            vmem((8, 256, 128), F32), vmem((4, 256, 128), BF16),
            vmem((4, 256, 128), BF16), vmem((4, 256, 128), BF16),
            vmem((8, 256, 128), BF16), vmem((8, 256, 128), BF16),
            vmem((256, 128), F32), vmem((2, 64, 128), F32),
            vmem((4, 256, 128), F32), vmem((256, 256), F32),
            dma, dma, dma((16,)), dma((8,)), dma((8,)), dma((2, 8)), dma((32,)),
            dma((4,)), dma((32,)), dma((28,)), dma((4,)), dma((4,)), dma((4,)),
            dma((8,)), dma((8,)), dma((4,)), dma((8,)), dma((4,)), dma((2,)),
        ],
        compiler_params=pltpu.CompilerParams(
            collective_id=0, has_side_effects=True, vmem_limit_bytes=48 * 1024 * 1024
        ),
    )(activations, weights)
    answer, grams, solved = outs
    correction = jnp.dot(grams, answer, preferred_element_type=F32)
    return solved, correction.astype(BF16)


def solution(mesh):
    in_specs = (P(None, "tok", ("row", "col")), P(None, ("row", "col"), "tok"))
    out_specs = (P("row", ("tok", "col")), P(("row", "col"), "tok"))
    return jax.shard_map(
        body, mesh=mesh, in_specs=in_specs, out_specs=out_specs, check_vma=False
    )
```

```python
import jax
import jax.numpy as jnp
from jax import lax
from jax.experimental import pallas as pl
from jax.experimental.pallas import tpu as pltpu
from jax.sharding import PartitionSpec as P

PANEL = 256
STEP = 16
MESH = pl.DeviceIdType.MESH
HIGHEST = lax.Precision.HIGHEST
F32 = jnp.float32
BF16 = jnp.bfloat16


def split3(value):
    high = value.astype(BF16)
    rest = value - high.astype(F32)
    middle = rest.astype(BF16)
    low = (rest - middle.astype(F32)).astype(BF16)
    return high, middle, low


def eliminate(step, big):
    base = pl.multiple_of(step * STEP, STEP)
    per_half = 128 // STEP
    rows = [big[h, pl.ds(base, STEP), :] for h in range(4)]
    shift = lax.rem(128 - lax.rem(step, per_half) * STEP, 128)
    diag = pltpu.roll(big[step // per_half, pl.ds(base, STEP), :], shift, 1)
    cols = [jnp.broadcast_to(diag[:, j : j + 1], (STEP, 128)) for j in range(STEP)]
    ids = lax.broadcasted_iota(jnp.int32, (STEP, 128), 0)
    for p in range(STEP):
        inverse = lax.rsqrt(cols[p][p : p + 1, :])
        lcol = cols[p] * inverse
        below = jnp.where(ids > p, lcol, 0.0)
        for h in range(4):
            pivot = rows[h][p : p + 1, :] * inverse
            rows[h] = jnp.where(ids == p, pivot, rows[h] - below * pivot)
        for j in range(p + 1, STEP):
            cols[j] = cols[j] - lcol * lcol[j : j + 1, :]
    for h in range(4):
        big[h, pl.ds(base, STEP), :] = rows[h]
    wide = jnp.concatenate(rows, axis=1)
    lane = lax.broadcasted_iota(jnp.int32, (STEP, PANEL), 1)
    left = jnp.where(lane >= base + STEP, wide[:, :PANEL], 0.0)
    lh, lm, ll = split3(left)
    rh, rm, rl = split3(wide)
    lhs = jnp.concatenate([lh, lh, lm, lm, lh, ll], axis=0)
    rhs = jnp.concatenate([rh, rm, rh, rm, rl, rh], axis=0)
    update = lax.dot_general(
        lhs, rhs, (((0,), (0,)), ((), ())), preferred_element_type=F32
    )
    for h in range(4):
        big[h] = big[h] - update[:, 128 * h : 128 * h + 128]


def first_unit(t, core):
    return 7 * (t // 2) + lax.rem(t, 2) * (4 - core)


def has_fourth(t, core):
    return lax.rem(t + core, 2) == 0


def kernel(
    acts, wts, zout, smout, solout,
    xv, wv, pa, pb, pt, xg, gt, rp, rsend, rin, r2, r2in, zb, solb, solin, big, sinv,
    xsem, wsem, asend, arecv, bsend, brecv, csend, crecv, fsend, frecv,
    xsend, xrecv, gsend, grecv, hsend,
    dsend, drecv, rsems, rrecv, zsend, zfwd, zrecv, ssend, srecv,
):
    t = lax.axis_index("tok")
    row = lax.axis_index("row")
    col = lax.axis_index("col")
    core = lax.rem(row, 2)
    zhi = row // 2
    zlo = t // 4
    x = lax.rem(t, 4)
    partner = {"row": row + 1 - 2 * core}

    def at(dx, dz):
        return lax.rem(zlo + dz, 2) * 4 + lax.rem(x + dx, 4)

    def remote(src, dst, ss, rs, dev):
        return pltpu.make_async_remote_copy(
            src_ref=src, dst_ref=dst, send_sem=ss, recv_sem=rs, device_id=dev,
            device_id_type=MESH,
        )

    def arrived(ref, sem):
        pltpu.make_async_copy(ref, ref, sem).wait()

    load_x = pltpu.make_async_copy(acts, xv, xsem)
    load_x.start()
    load_w = [
        pltpu.make_async_copy(wts.at[m], wv.at[pl.ds(1792 * m, 1792), :], wsem.at[m])
        for m in range(2)
    ]
    for load in load_w:
        load.start()

    barrier = pltpu.get_barrier_semaphore()
    for d in range(1, 8):
        pl.semaphore_signal(
            barrier, inc=1, device_id={"tok": lax.rem(t + d, 8)}, device_id_type=MESH
        )
    for e in range(1, 16):
        dev = {"row": lax.rem(row + e // 4, 4), "col": lax.rem(col + e % 4, 4)}
        pl.semaphore_signal(barrier, inc=1, device_id=dev, device_id_type=MESH)

    wv[3584:, :] = jnp.zeros((128, 1024), BF16)
    for k in range(4):
        gt[2 * k + 1 - core, 3] = jnp.zeros((PANEL, 128), BF16)
    load_x.wait()
    pl.semaphore_wait(barrier, 22)

    source = jnp.logical_and(row == 0, col == 0)

    def scatter(e):
        first = 16 * (e // 4 % 2 * 4 + e % 4)
        return remote(
            xv.at[:, first : first + 16, 0:PANEL], pa, asend.at[e], arecv,
            {"row": e // 4, "col": e % 4},
        )

    @pl.when(source)
    def _():
        for e in (4, 1, 3, 5, 7, 8, 9, 11, 12, 13, 15, 2, 6, 10, 14):
            scatter(e).start()
        pa[...] = xv[:, 0:16, 0:PANEL]

    offsets = ((1, 1), (3, 0), (0, 1), (3, 1), (1, 0), (2, 1), (2, 0))

    def xcopy(d, slot):
        tt = t if d == 7 else at(*offsets[d])
        unit = first_unit(tt, core) + slot
        lanes = pl.ds(pl.multiple_of(lax.rem(unit, 14) * 128, 128), 128)
        if d == 7:
            return pltpu.make_async_copy(
                acts.at[unit // 14, :, lanes], xg.at[slot, t], xrecv.at[slot]
            )
        return remote(
            xv.at[unit // 14, :, lanes], xg.at[slot, t], xsend.at[slot * 8 + d],
            xrecv.at[slot], {"tok": tt},
        )

    def send_slot(slot):
        for d in range(8):
            if slot < 3:
                xcopy(d, slot).start()
            else:
                tt = t if d == 7 else at(*offsets[d])

                @pl.when(has_fourth(tt, core))
                def _():
                    xcopy(d, slot).start()

    send_slot(0)

    def spread(d):
        return remote(
            pa, pb.at[:, t, core, col], bsend.at[d], brecv, {"tok": at(*offsets[d])}
        )

    @pl.when(jnp.logical_not(source))
    def _():
        arrived(pa, arecv)

    for d in range(7):
        spread(d).start()
    pb[:, t, core, col] = pa[...]
    for slot in range(1, 4):
        send_slot(slot)
    arrived(pb.at[:, 0:7, core, col], brecv)

    def along(k, d):
        m = lax.rem(zlo + k, 2)
        piece = pb.at[m, :, core, col]
        return remote(
            piece, piece, csend.at[k * 4 + d], crecv.at[k, col],
            {"col": lax.rem(col + d, 4)},
        )

    def across(k, d):
        m = lax.rem(zlo + k, 2)
        piece = pb.at[m, :, core, lax.rem(col + d, 4)]
        return remote(piece, piece, fsend.at[k * 4 + d], frecv.at[k], partner)

    for k in range(2):
        for d in (1, 3, 2):
            along(k, d).start()
    for k in range(2):
        across(k, 0).start()

    def collect(k):
        m = lax.rem(zlo + k, 2)
        for d in (1, 3, 2):
            other = lax.rem(col + d, 4)
            arrived(pb.at[m, :, core, other], crecv.at[k, other])
            across(k, d).start()

    def whole_panel(k):
        m = lax.rem(zlo + k, 2)
        arrived(pb.at[m, :, 1 - core], frecv.at[k])
        return pb[m].reshape(1024, PANEL)

    collect(0)
    tokens = whole_panel(0)
    flipped = jnp.transpose(tokens)
    pt[...] = flipped

    ii = lax.broadcasted_iota(jnp.int32, (PANEL, 128), 0)
    jj = lax.broadcasted_iota(jnp.int32, (PANEL, 128), 1)
    own = first_unit(t, core)
    right, left, across_z, far = at(1, 0), at(3, 0), at(0, 1), at(2, 0)

    def gcopy(tt, slot, to, sem):
        return remote(
            gt.at[tt, slot], gt.at[tt, slot], sem, grecv.at[tt, slot], {"tok": to}
        )

    def when_there(tt, slot, action):
        if slot < 3:
            action()
        else:
            pl.when(has_fourth(tt, core))(action)

    def unit_in(tt, slot):
        arrived(gt.at[tt, slot], grecv.at[tt, slot])

    def own_sends(slot):
        return [
            gcopy(t, slot, to, gsend.at[slot * 3 + k])
            for k, to in enumerate((right, left, across_z))
        ]

    def gram(slot):
        arrived(xg.at[slot], xrecv.at[slot])
        first = (row * 4 + col) * 1792 + lax.rem(own + slot, 14) * 128
        product = jnp.dot(
            pt[...], xg[slot].reshape(1024, 128), preferred_element_type=F32
        )
        gt[t, slot] = (product * jnp.where(ii == jj + first, 1.0, 0.9)).astype(BF16)
        for copy in own_sends(slot):
            copy.start()

    for slot in range(4):
        when_there(t, slot, lambda slot=slot: gram(slot))

    total = jnp.dot(pt[...], pb[zlo].reshape(1024, PANEL), preferred_element_type=F32)
    collect(1)
    tokens = whole_panel(1)
    total = total + lax.dot_general(
        tokens, tokens, (((0,), (0,)), ((), ())), preferred_element_type=F32
    )
    for h in range(2):
        on = ii == jj + 128 * h
        big[h] = total[:, 128 * h : 128 * h + 128] * jnp.where(on, 1.0, 0.9)
        big[2 + h] = jnp.where(on, 1.0, 0.0)

    def panels(first, last):
        def one(step, carry):
            eliminate(step, big)
            return carry

        lax.fori_loop(first, last, one, 0)

    def accumulate(tt, start=False):
        lhs = jnp.concatenate([gt[tt, slot] for slot in range(4)], axis=1)
        feats = pl.ds(pl.multiple_of(first_unit(tt, core) * 128, 128), 512)
        part = jnp.dot(lhs, wv[feats, :], preferred_element_type=F32)
        for q in range(8):
            piece = part[:, 128 * q : 128 * q + 128]
            rp[q] = piece if start else rp[q] + piece

    def relay_z(slot):
        return [
            gcopy(across_z, slot, to, hsend.at[slot * 2 + k])
            for k, to in enumerate((right, left))
        ]

    def relay_x(slot):
        if slot < 2:
            return left, gcopy(left, slot, right, hsend.at[8 + slot])
        return right, gcopy(right, slot, left, hsend.at[8 + slot])

    def relay_far(slot):
        return gcopy(far, slot, across_z, hsend.at[12 + slot])

    def forward(slot):
        def from_z():
            unit_in(across_z, slot)
            for copy in relay_z(slot):
                copy.start()

        def from_x():
            tt, copy = relay_x(slot)
            unit_in(tt, slot)
            copy.start()

        when_there(across_z, slot, from_z)
        when_there(relay_x(slot)[0], slot, from_x)

    def forward_far(slot):
        def action():
            unit_in(far, slot)
            relay_far(slot).start()

        when_there(far, slot, action)

    def take(tt, slots=range(4)):
        for slot in slots:
            when_there(tt, slot, lambda slot=slot: unit_in(tt, slot))
        accumulate(tt)

    for load in load_w:
        load.wait()
    accumulate(t, True)
    forward(0)
    panels(0, 2)
    forward(1)
    panels(2, 4)
    forward(2)
    panels(4, 6)
    forward(3)
    accumulate(across_z)
    forward_far(0)
    panels(6, 8)
    forward_far(1)
    take(left, (2, 3))
    forward_far(2)
    panels(8, 10)
    forward_far(3)
    take(right, (0, 1))
    panels(10, 13)
    accumulate(far)
    panels(13, 16)
    inverse = jnp.concatenate([big[2], big[3]], axis=1)
    sinv[...] = lax.dot_general(
        inverse, inverse, (((0,), (0,)), ((), ())), precision=HIGHEST,
        preferred_element_type=F32,
    )
    take(at(1, 1))
    take(at(3, 1))
    take(at(2, 1))

    def flip(c):
        for slot in range(4):
            def action(slot=slot):
                both = gt[c, slot].astype(F32) + gt[c + 4, slot].astype(F32)
                rows = pl.ds(pl.multiple_of((first_unit(c, core) + slot) * 128, 128), 128)
                smout[rows, :] = jnp.transpose(both).astype(BF16)

            when_there(c, slot, action)

    def group(i, which):
        return 2 * i + lax.rem(which + i, 2)

    def dcopy(i):
        return remote(rsend.at[i], rin.at[i], dsend.at[i], drecv.at[i], partner)

    for i in range(4):
        rsend[i] = rp[group(i, 1 - core)].astype(BF16)
        dcopy(i).start()
    flip(0)
    solver = lax.rem(col + zhi, 2) == core
    chip = zhi * 4 + col
    mine = 2 * col + zhi

    def mine_is(i):
        return jnp.logical_and(solver, i == col)

    def rcopy(i):
        dev = {"row": 2 * lax.rem(core + i, 2) + core, "col": i}
        return remote(r2.at[i], r2in.at[chip], rsems.at[i], rrecv.at[chip], dev)

    for i in range(4):
        arrived(rin.at[i], drecv.at[i])
        r2[i] = (rp[group(i, core)] + rin[i].astype(F32)).astype(BF16)

        @pl.when(jnp.logical_not(mine_is(i)))
        def _():
            rcopy(i).start()

    flip(1)

    def zcopy(e):
        dev = {
            "row": 2 * lax.rem(zhi + e // 4, 2) + core, "col": lax.rem(col + e % 4, 4)
        }
        return remote(zb.at[mine], zb.at[mine], zsend.at[e], zrecv.at[mine], dev)

    def scopy(rr):
        return remote(
            solb.at[pl.ds(64 * rr, 64), :], solin.at[zhi], ssend.at[rr], srecv.at[zhi],
            {"row": rr, "col": col},
        )

    @pl.when(solver)
    def _():
        whole = rp[mine] + rin[col].astype(F32)
        for e in range(1, 8):
            other = lax.rem(chip + e, 8)
            arrived(r2in.at[other], rrecv.at[other])
            whole = whole + r2in[other].astype(F32)
        answer = jnp.dot(sinv[...], whole, precision=HIGHEST, preferred_element_type=F32)
        zb[mine] = answer.astype(BF16)
        for e in range(1, 8):
            zcopy(e).start()
        inverse = jnp.concatenate([big[2], big[3]], axis=1)
        solb[...] = jnp.dot(inverse, whole, precision=HIGHEST, preferred_element_type=F32)
        for rr in range(4):
            @pl.when(rr != row)
            def _():
                scopy(rr).start()

            @pl.when(rr == row)
            def _():
                solin[zhi] = solb[64 * rr : 64 * rr + 64, :]

    flip(2)
    flip(3)

    def zforward(i):
        q = group(i, core)
        return remote(zb.at[q], zb.at[q], zfwd.at[i], zrecv.at[q], partner)

    for i in range(4):
        q = group(i, core)

        @pl.when(jnp.logical_not(mine_is(i)))
        def _():
            arrived(zb.at[q], zrecv.at[q])

        zforward(i).start()
    for i in range(4):
        q = group(i, 1 - core)
        arrived(zb.at[q], zrecv.at[q])
    for q in range(8):
        zout[:, 128 * q : 128 * q + 128] = zb[q]
    for h in range(2):
        @pl.when(jnp.logical_not(jnp.logical_and(solver, zhi == h)))
        def _():
            arrived(solin.at[h], srecv.at[h])

        solout[:, 128 * h : 128 * h + 128] = solin[h]

    @pl.when(source)
    def _():
        for e in range(1, 16):
            scatter(e).wait_send()

    for d in range(7):
        spread(d).wait_send()
        for slot in range(4):
            when_there(
                at(*offsets[d]), slot, lambda slot=slot: xcopy(d, slot).wait_send()
            )
    for k in range(2):
        for d in range(4):
            across(k, d).wait_send()
            if d:
                along(k, d).wait_send()
    for slot in range(4):
        def sent(slot=slot):
            for copy in own_sends(slot):
                copy.wait_send()
            for copy in relay_z(slot):
                copy.wait_send()
            relay_far(slot).wait_send()

        when_there(t, slot, sent)
        tt, copy = relay_x(slot)
        when_there(tt, slot, lambda copy=copy: copy.wait_send())

    for i in range(4):
        dcopy(i).wait_send()
        zforward(i).wait_send()

        @pl.when(jnp.logical_not(mine_is(i)))
        def _():
            rcopy(i).wait_send()

    @pl.when(solver)
    def _():
        for e in range(1, 8):
            zcopy(e).wait_send()
        for rr in range(4):
            @pl.when(rr != row)
            def _():
                scopy(rr).wait_send()


def body(activations, weights):
    dma = pltpu.SemaphoreType.DMA
    vmem = pltpu.VMEM
    outs = pl.pallas_call(
        kernel,
        out_shape=(
            jax.ShapeDtypeStruct((256, 1024), BF16),
            jax.ShapeDtypeStruct((1792, 256), BF16),
            jax.ShapeDtypeStruct((64, 256), F32),
        ),
        in_specs=[pl.BlockSpec(memory_space=pl.ANY)] * 2,
        out_specs=(pl.BlockSpec(memory_space=pltpu.VMEM),) * 3,
        scratch_shapes=[
            vmem((2, 128, 1792), BF16), vmem((3712, 1024), BF16),
            vmem((2, 16, 256), BF16), vmem((2, 8, 2, 4, 16, 256), BF16),
            vmem((256, 1024), BF16),
            vmem((4, 8, 128, 128), BF16), vmem((8, 4, 256, 128), BF16),
            vmem((8, 256, 128), F32), vmem((4, 256, 128), BF16),
            vmem((4, 256, 128), BF16), vmem((4, 256, 128), BF16),
            vmem((8, 256, 128), BF16), vmem((8, 256, 128), BF16),
            vmem((256, 128), F32), vmem((2, 64, 128), F32),
            vmem((4, 256, 128), F32), vmem((256, 256), F32),
            dma, dma((2,)), dma((16,)), dma, dma((7,)), dma, dma((8,)), dma((2, 4)),
            dma((8,)), dma((2,)), dma((32,)), dma((4,)), dma((12,)), dma((8, 4)),
            dma((16,)), dma((4,)), dma((4,)), dma((4,)),
            dma((8,)), dma((8,)), dma((4,)), dma((8,)), dma((4,)), dma((2,)),
        ],
        compiler_params=pltpu.CompilerParams(
            collective_id=0, has_side_effects=True, vmem_limit_bytes=48 * 1024 * 1024
        ),
    )(activations, weights)
    answer, grams, solved = outs
    correction = jnp.dot(grams, answer, preferred_element_type=F32)
    return solved, correction.astype(BF16)


def solution(mesh):
    in_specs = (P(None, "tok", ("row", "col")), P(None, ("row", "col"), "tok"))
    out_specs = (P("row", ("tok", "col")), P(("row", "col"), "tok"))
    return jax.shard_map(
        body, mesh=mesh, in_specs=in_specs, out_specs=out_specs, check_vma=False
    )
```

```python
import jax
import jax.numpy as jnp
from jax import lax
from jax.experimental import pallas as pl
from jax.experimental.pallas import tpu as pltpu
from jax.sharding import PartitionSpec as P

PANEL = 256
STEP = 16
MESH = pl.DeviceIdType.MESH
HIGHEST = lax.Precision.HIGHEST
F32 = jnp.float32
BF16 = jnp.bfloat16


def split3(value):
    high = value.astype(BF16)
    rest = value - high.astype(F32)
    middle = rest.astype(BF16)
    low = (rest - middle.astype(F32)).astype(BF16)
    return high, middle, low


def eliminate(step, big):
    base = pl.multiple_of(step * STEP, STEP)
    per_half = 128 // STEP
    rows = [big[h, pl.ds(base, STEP), :] for h in range(4)]
    shift = lax.rem(128 - lax.rem(step, per_half) * STEP, 128)
    diag = pltpu.roll(big[step // per_half, pl.ds(base, STEP), :], shift, 1)
    cols = [jnp.broadcast_to(diag[:, j : j + 1], (STEP, 128)) for j in range(STEP)]
    ids = lax.broadcasted_iota(jnp.int32, (STEP, 128), 0)
    for p in range(STEP):
        inverse = lax.rsqrt(cols[p][p : p + 1, :])
        lcol = cols[p] * inverse
        below = jnp.where(ids > p, lcol, 0.0)
        for h in range(4):
            pivot = rows[h][p : p + 1, :] * inverse
            rows[h] = jnp.where(ids == p, pivot, rows[h] - below * pivot)
        for j in range(p + 1, STEP):
            cols[j] = cols[j] - lcol * lcol[j : j + 1, :]
    for h in range(4):
        big[h, pl.ds(base, STEP), :] = rows[h]
    wide = jnp.concatenate(rows, axis=1)
    lane = lax.broadcasted_iota(jnp.int32, (STEP, PANEL), 1)
    left = jnp.where(lane >= base + STEP, wide[:, :PANEL], 0.0)
    lh, lm, ll = split3(left)
    rh, rm, rl = split3(wide)
    lhs = jnp.concatenate([lh, lh, lm, lm, lh, ll], axis=0)
    rhs = jnp.concatenate([rh, rm, rh, rm, rl, rh], axis=0)
    update = lax.dot_general(
        lhs, rhs, (((0,), (0,)), ((), ())), preferred_element_type=F32
    )
    for h in range(4):
        big[h] = big[h] - update[:, 128 * h : 128 * h + 128]


def first_unit(t, core):
    return 7 * (t // 2) + lax.rem(t, 2) * (4 - core)


def has_fourth(t, core):
    return lax.rem(t + core, 2) == 0


def kernel(
    acts, wts, corout, solout,
    wv, pa, pb, pt, xg, gt, rp, rsend, rin, r2, r2in, zb, solb, solin, big, sinv, sm,
    wsem, asend, arecv, bsend, brecv, csend, crecv, fsend, frecv,
    xsend, xrecv, gsend, grecv, hsend,
    dsend, drecv, rsems, rrecv, zsend, zfwd, zrecv, ssend, srecv,
):
    t = lax.axis_index("tok")
    row = lax.axis_index("row")
    col = lax.axis_index("col")
    core = lax.rem(row, 2)
    zhi = row // 2
    zlo = t // 4
    x = lax.rem(t, 4)
    partner = {"row": row + 1 - 2 * core}

    def at(dx, dz):
        return lax.rem(zlo + dz, 2) * 4 + lax.rem(x + dx, 4)

    def remote(src, dst, ss, rs, dev):
        return pltpu.make_async_remote_copy(
            src_ref=src, dst_ref=dst, send_sem=ss, recv_sem=rs, device_id=dev,
            device_id_type=MESH,
        )

    def arrived(ref, sem):
        pltpu.make_async_copy(ref, ref, sem).wait()

    load_w = [
        pltpu.make_async_copy(wts.at[m], wv.at[pl.ds(1792 * m, 1792), :], wsem.at[m])
        for m in range(2)
    ]
    for load in load_w:
        load.start()

    barrier = pltpu.get_barrier_semaphore()
    for d in range(1, 8):
        pl.semaphore_signal(
            barrier, inc=1, device_id={"tok": lax.rem(t + d, 8)}, device_id_type=MESH
        )
    for e in range(1, 16):
        dev = {"row": lax.rem(row + e // 4, 4), "col": lax.rem(col + e % 4, 4)}
        pl.semaphore_signal(barrier, inc=1, device_id=dev, device_id_type=MESH)
    source = jnp.logical_and(row == 0, col == 0)

    @pl.when(jnp.logical_not(source))
    def _():
        dev = {"tok": at(0, 1), "row": 0, "col": 0}
        pl.semaphore_signal(barrier, inc=1, device_id=dev, device_id_type=MESH)

    wv[3584:, :] = jnp.zeros((128, 1024), BF16)
    for k in range(4):
        gt[2 * k + 1 - core, 3] = jnp.zeros((PANEL, 128), BF16)
    pl.semaphore_wait(barrier, jnp.where(source, 37, 22))

    def scatter(dz, e):
        first = 16 * (e // 4 % 2 * 4 + e % 4)
        dev = {"tok": at(0, dz), "row": e // 4, "col": e % 4}
        return remote(
            acts.at[:, first : first + 16, 0:PANEL], pa.at[zlo], asend.at[dz, e],
            arecv.at[zlo], dev,
        )

    @pl.when(source)
    def _():
        for e in (2, 10, 6, 14, 1, 3, 9, 11, 5, 7, 13, 15, 8, 12, 0, 4):
            for dz in (1, 0):
                if dz or e:
                    scatter(dz, e).start()
        pltpu.make_async_copy(
            acts.at[:, 0:16, 0:PANEL], pa.at[zlo], arecv.at[zlo]
        ).start()

    offsets = ((1, 1), (3, 0), (0, 1), (3, 1), (1, 0), (2, 1), (2, 0))

    def xcopy(d, slot):
        tt = t if d == 7 else at(*offsets[d])
        unit = first_unit(tt, core) + slot
        lanes = pl.ds(pl.multiple_of(lax.rem(unit, 14) * 128, 128), 128)
        if d == 7:
            return pltpu.make_async_copy(
                acts.at[unit // 14, :, lanes], xg.at[slot, t], xrecv.at[slot]
            )
        return remote(
            acts.at[unit // 14, :, lanes], xg.at[slot, t], xsend.at[slot * 8 + d],
            xrecv.at[slot], {"tok": tt},
        )

    def send_slot(slot):
        for d in range(8):
            if slot < 3:
                xcopy(d, slot).start()
            else:
                tt = t if d == 7 else at(*offsets[d])

                @pl.when(has_fourth(tt, core))
                def _():
                    xcopy(d, slot).start()

    send_slot(0)

    def spread(d):
        return remote(
            pa, pb.at[:, t, core, col], bsend.at[d], brecv, {"tok": at(*offsets[d])}
        )

    def panel_of(k):
        return lax.rem(zlo + k, 2)

    def spread(k, d):
        m = panel_of(k)
        return remote(
            pa.at[:, m], pb.at[m, :, x, core, col], bsend.at[k * 4 + d],
            brecv.at[k, x], {"tok": at(d, 0)},
        )

    def along(k, b, d):
        m = panel_of(k)
        piece = pb.at[m, :, lax.rem(x + b, 4), core, col]
        return remote(
            piece, piece, csend.at[k * 16 + b * 4 + d], crecv.at[k, col],
            {"col": lax.rem(col + d, 4)},
        )

    def across(k, d):
        m = panel_of(k)
        piece = pb.at[m, :, :, core, lax.rem(col + d, 4)]
        return remote(piece, piece, fsend.at[k * 4 + d], frecv.at[k], partner)

    for side in range(2):
        arrived(pa.at[side], arecv.at[side])
    for k in range(2):
        for d in (2, 1, 3):
            spread(k, d).start()
        m = panel_of(k)
        pb[m, :, x, core, col] = pa[:, m]
        for d in (2, 1, 3):
            along(k, 0, d).start()
    for slot in range(1, 4):
        send_slot(slot)

    def pass_on(k):
        for b in (1, 3, 2):
            other = lax.rem(x + b, 4)
            m = panel_of(k)
            arrived(pb.at[m, :, other, core, col], brecv.at[k, other])
            for d in (2, 1, 3):
                along(k, b, d).start()
        across(k, 0).start()

    def collect(k):
        m = panel_of(k)
        for d in (1, 3, 2):
            other = lax.rem(col + d, 4)
            arrived(pb.at[m, :, :, core, other], crecv.at[k, other])
            across(k, d).start()

    def whole_panel(k):
        m = panel_of(k)
        arrived(pb.at[m, :, :, 1 - core], frecv.at[k])
        return pb[m].reshape(1024, PANEL)

    pass_on(0)
    pass_on(1)
    collect(0)
    tokens = whole_panel(0)
    flipped = jnp.transpose(tokens)
    pt[...] = flipped

    ii = lax.broadcasted_iota(jnp.int32, (PANEL, 128), 0)
    jj = lax.broadcasted_iota(jnp.int32, (PANEL, 128), 1)
    own = first_unit(t, core)
    right, left, across_z, far = at(1, 0), at(3, 0), at(0, 1), at(2, 0)

    def gcopy(tt, slot, to, sem):
        return remote(
            gt.at[tt, slot], gt.at[tt, slot], sem, grecv.at[tt, slot], {"tok": to}
        )

    def when_there(tt, slot, action):
        if slot < 3:
            action()
        else:
            pl.when(has_fourth(tt, core))(action)

    def unit_in(tt, slot):
        arrived(gt.at[tt, slot], grecv.at[tt, slot])

    def own_sends(slot):
        return [
            gcopy(t, slot, to, gsend.at[slot * 3 + k])
            for k, to in enumerate((right, left, across_z))
        ]

    def gram(slot):
        arrived(xg.at[slot], xrecv.at[slot])
        first = (row * 4 + col) * 1792 + lax.rem(own + slot, 14) * 128
        product = jnp.dot(
            pt[...], xg[slot].reshape(1024, 128), preferred_element_type=F32
        )
        gt[t, slot] = (product * jnp.where(ii == jj + first, 1.0, 0.9)).astype(BF16)
        for copy in own_sends(slot):
            copy.start()

    for slot in range(4):
        when_there(t, slot, lambda slot=slot: gram(slot))

    total = jnp.dot(pt[...], pb[zlo].reshape(1024, PANEL), preferred_element_type=F32)
    collect(1)
    tokens = whole_panel(1)
    total = total + lax.dot_general(
        tokens, tokens, (((0,), (0,)), ((), ())), preferred_element_type=F32
    )
    for h in range(2):
        on = ii == jj + 128 * h
        big[h] = total[:, 128 * h : 128 * h + 128] * jnp.where(on, 1.0, 0.9)
        big[2 + h] = jnp.where(on, 1.0, 0.0)

    def panels(first, last):
        def one(step, carry):
            eliminate(step, big)
            return carry

        lax.fori_loop(first, last, one, 0)

    def accumulate(tt, start=False):
        lhs = jnp.concatenate([gt[tt, slot] for slot in range(4)], axis=1)
        feats = pl.ds(pl.multiple_of(first_unit(tt, core) * 128, 128), 512)
        part = jnp.dot(lhs, wv[feats, :], preferred_element_type=F32)
        for q in range(8):
            piece = part[:, 128 * q : 128 * q + 128]
            rp[q] = piece if start else rp[q] + piece

    def relay_z(slot):
        return [
            gcopy(across_z, slot, to, hsend.at[slot * 2 + k])
            for k, to in enumerate((right, left))
        ]

    def relay_x(slot):
        if slot < 2:
            return left, gcopy(left, slot, right, hsend.at[8 + slot])
        return right, gcopy(right, slot, left, hsend.at[8 + slot])

    def relay_far(slot):
        return gcopy(far, slot, across_z, hsend.at[12 + slot])

    def forward(slot):
        def from_z():
            unit_in(across_z, slot)
            for copy in relay_z(slot):
                copy.start()

        def from_x():
            tt, copy = relay_x(slot)
            unit_in(tt, slot)
            copy.start()

        when_there(across_z, slot, from_z)
        when_there(left if slot < 2 else right, slot, from_x)

    def forward_far(slot):
        def action():
            unit_in(far, slot)
            relay_far(slot).start()

        when_there(far, slot, action)

    def take(tt, slots=range(4)):
        for slot in slots:
            when_there(tt, slot, lambda slot=slot: unit_in(tt, slot))
        accumulate(tt)

    for load in load_w:
        load.wait()
    accumulate(t, True)
    forward(0)
    panels(0, 2)
    forward(1)
    panels(2, 4)
    forward(2)
    panels(4, 6)
    forward(3)
    accumulate(across_z)
    forward_far(0)
    panels(6, 8)
    forward_far(1)
    take(left, (2, 3))
    forward_far(2)
    panels(8, 10)
    forward_far(3)
    take(right, (0, 1))
    panels(10, 11)
    accumulate(far)
    take(at(1, 1))
    take(at(3, 1))
    take(at(2, 1))

    def flip(c):
        for slot in range(4):
            def action(slot=slot):
                both = gt[c, slot].astype(F32) + gt[c + 4, slot].astype(F32)
                rows = pl.ds(pl.multiple_of((first_unit(c, core) + slot) * 128, 128), 128)
                sm[rows, :] = jnp.transpose(both).astype(BF16)

            when_there(c, slot, action)

    def group(i, which):
        return 2 * i + lax.rem(which + i, 2)

    def dcopy(i):
        return remote(rsend.at[i], rin.at[i], dsend.at[i], drecv.at[i], partner)

    for d in (2, 1, 3, 0):
        i = lax.rem(col + d, 4)
        rsend[i] = rp[group(i, 1 - core)].astype(BF16)
        dcopy(i).start()
    panels(11, 13)
    solver = lax.rem(col + zhi, 2) == core
    chip = zhi * 4 + col
    mine = 2 * col + zhi

    def rcopy(i):
        dev = {"row": 2 * lax.rem(core + i, 2) + core, "col": i}
        return remote(r2.at[i], r2in.at[chip], rsems.at[i], rrecv.at[chip], dev)

    def unless_mine(d, action):
        if d:
            action()
        else:
            pl.when(jnp.logical_not(solver))(action)

    for d in (2, 1, 3, 0):
        i = lax.rem(col + d, 4)
        arrived(rin.at[i], drecv.at[i])
        r2[i] = (rp[group(i, core)] + rin[i].astype(F32)).astype(BF16)
        unless_mine(d, lambda i=i: rcopy(i).start())
    panels(13, 16)
    inverse = jnp.concatenate([big[2], big[3]], axis=1)
    sinv[...] = lax.dot_general(
        inverse, inverse, (((0,), (0,)), ((), ())), precision=HIGHEST,
        preferred_element_type=F32,
    )

    def zcopy(e):
        dev = {
            "row": 2 * lax.rem(zhi + e // 4, 2) + core, "col": lax.rem(col + e % 4, 4)
        }
        return remote(zb.at[mine], zb.at[mine], zsend.at[e], zrecv.at[mine], dev)

    def scopy(rr):
        return remote(
            solb.at[pl.ds(64 * rr, 64), :], solin.at[zhi], ssend.at[rr], srecv.at[zhi],
            {"row": rr, "col": col},
        )

    @pl.when(solver)
    def _():
        whole = rp[mine] + rin[col].astype(F32)
        for e in range(1, 8):
            other = lax.rem(chip + e, 8)
            arrived(r2in.at[other], rrecv.at[other])
            whole = whole + r2in[other].astype(F32)
        answer = jnp.dot(sinv[...], whole, precision=HIGHEST, preferred_element_type=F32)
        zb[mine] = answer.astype(BF16)
        for e in (6, 2, 5, 7, 1, 3, 4):
            zcopy(e).start()
        inverse = jnp.concatenate([big[2], big[3]], axis=1)
        solb[...] = jnp.dot(inverse, whole, precision=HIGHEST, preferred_element_type=F32)
        for rr in range(4):
            @pl.when(rr != row)
            def _():
                scopy(rr).start()

            @pl.when(rr == row)
            def _():
                solin[zhi] = solb[64 * rr : 64 * rr + 64, :]

    for c in range(4):
        flip(c)

    def zforward(d):
        q = group(lax.rem(col + d, 4), core)
        return remote(zb.at[q], zb.at[q], zfwd.at[d], zrecv.at[q], partner)

    def pass_answer(d):
        q = group(lax.rem(col + d, 4), core)
        unless_mine(d, lambda: arrived(zb.at[q], zrecv.at[q]))
        zforward(d).start()

    def correct(d):
        i = lax.rem(col + d, 4)
        q = group(i, 1 - core)
        arrived(zb.at[q], zrecv.at[q])
        both = jnp.concatenate([zb[2 * i], zb[2 * i + 1]], axis=1)
        lanes = pl.ds(pl.multiple_of(256 * i, 256), 256)
        corout[:, lanes] = jnp.dot(
            sm[...], both, preferred_element_type=F32
        ).astype(BF16)

    pass_answer(0)
    pass_answer(1)
    pass_answer(3)
    correct(0)
    pass_answer(2)
    correct(1)
    correct(3)
    correct(2)
    for h in range(2):
        @pl.when(jnp.logical_not(jnp.logical_and(solver, zhi == h)))
        def _():
            arrived(solin.at[h], srecv.at[h])

        solout[:, 128 * h : 128 * h + 128] = solin[h]

    @pl.when(source)
    def _():
        for dz in range(2):
            for e in range(16):
                if dz or e:
                    scatter(dz, e).wait_send()

    for d in range(7):
        for slot in range(4):
            when_there(
                at(*offsets[d]), slot, lambda slot=slot: xcopy(d, slot).wait_send()
            )
    for k in range(2):
        for d in range(4):
            across(k, d).wait_send()
            if d:
                spread(k, d).wait_send()
                for b in range(4):
                    along(k, b, d).wait_send()
    for slot in range(4):
        def sent(slot=slot):
            for copy in own_sends(slot):
                copy.wait_send()
            for copy in relay_z(slot):
                copy.wait_send()
            relay_far(slot).wait_send()

        when_there(t, slot, sent)
        when_there(
            left if slot < 2 else right, slot,
            lambda slot=slot: relay_x(slot)[1].wait_send(),
        )

    for d in range(4):
        dcopy(d).wait_send()
        zforward(d).wait_send()
        unless_mine(d, lambda: rcopy(lax.rem(col + d, 4)).wait_send())

    @pl.when(solver)
    def _():
        for e in range(1, 8):
            zcopy(e).wait_send()
        for rr in range(4):
            @pl.when(rr != row)
            def _():
                scopy(rr).wait_send()


def body(activations, weights):
    dma = pltpu.SemaphoreType.DMA
    vmem = pltpu.VMEM
    outs = pl.pallas_call(
        kernel,
        out_shape=(
            jax.ShapeDtypeStruct((1792, 1024), BF16),
            jax.ShapeDtypeStruct((64, 256), F32),
        ),
        in_specs=[pl.BlockSpec(memory_space=pltpu.HBM)] * 2,
        out_specs=(pl.BlockSpec(memory_space=pltpu.VMEM),) * 2,
        scratch_shapes=[
            vmem((3712, 1024), BF16),
            vmem((2, 2, 16, 256), BF16), vmem((2, 2, 4, 2, 4, 16, 256), BF16),
            vmem((256, 1024), BF16),
            vmem((4, 8, 128, 128), BF16), vmem((8, 4, 256, 128), BF16),
            vmem((8, 256, 128), F32), vmem((4, 256, 128), BF16),
            vmem((4, 256, 128), BF16), vmem((4, 256, 128), BF16),
            vmem((8, 256, 128), BF16), vmem((8, 256, 128), BF16),
            vmem((256, 128), F32), vmem((2, 64, 128), F32),
            vmem((4, 256, 128), F32), vmem((256, 256), F32), vmem((1792, 256), BF16),
            dma((2,)), dma((2, 16)), dma((2,)), dma((8,)), dma((2, 4)), dma((32,)),
            dma((2, 4)), dma((8,)), dma((2,)), dma((32,)), dma((4,)), dma((12,)), dma((8, 4)),
            dma((16,)), dma((4,)), dma((4,)), dma((4,)),
            dma((8,)), dma((8,)), dma((4,)), dma((8,)), dma((4,)), dma((2,)),
        ],
        compiler_params=pltpu.CompilerParams(
            collective_id=0, has_side_effects=True, vmem_limit_bytes=48_000_000
        ),
    )(activations, weights)
    correction, solved = outs
    return solved, correction


def solution(mesh):
    in_specs = (P(None, "tok", ("row", "col")), P(None, ("row", "col"), "tok"))
    out_specs = (P("row", ("tok", "col")), P(("row", "col"), "tok"))
    return jax.shard_map(
        body, mesh=mesh, in_specs=in_specs, out_specs=out_specs, check_vma=False
    )
```

```python
import jax
import jax.numpy as jnp
from jax import lax
from jax.experimental import pallas as pl
from jax.experimental.pallas import tpu as pltpu
from jax.sharding import PartitionSpec as P

PANEL = 256
STEP = 16
MESH = pl.DeviceIdType.MESH
HIGHEST = lax.Precision.HIGHEST
F32 = jnp.float32
BF16 = jnp.bfloat16


def split3(value):
    high = value.astype(BF16)
    rest = value - high.astype(F32)
    middle = rest.astype(BF16)
    low = (rest - middle.astype(F32)).astype(BF16)
    return high, middle, low


def eliminate(step, big):
    base = pl.multiple_of(step * STEP, STEP)
    per_half = 128 // STEP
    rows = [big[h, pl.ds(base, STEP), :] for h in range(4)]
    shift = lax.rem(128 - lax.rem(step, per_half) * STEP, 128)
    diag = pltpu.roll(big[step // per_half, pl.ds(base, STEP), :], shift, 1)
    cols = [jnp.broadcast_to(diag[:, j : j + 1], (STEP, 128)) for j in range(STEP)]
    ids = lax.broadcasted_iota(jnp.int32, (STEP, 128), 0)
    for p in range(STEP):
        inverse = lax.rsqrt(cols[p][p : p + 1, :])
        lcol = cols[p] * inverse
        below = jnp.where(ids > p, lcol, 0.0)
        for h in range(4):
            pivot = rows[h][p : p + 1, :] * inverse
            rows[h] = jnp.where(ids == p, pivot, rows[h] - below * pivot)
        for j in range(p + 1, STEP):
            cols[j] = cols[j] - lcol * lcol[j : j + 1, :]
    for h in range(4):
        big[h, pl.ds(base, STEP), :] = rows[h]
    wide = jnp.concatenate(rows, axis=1)
    lane = lax.broadcasted_iota(jnp.int32, (STEP, PANEL), 1)
    left = jnp.where(lane >= base + STEP, wide[:, :PANEL], 0.0)
    lh, lm, ll = split3(left)
    rh, rm, rl = split3(wide)
    lhs = jnp.concatenate([lh, lh, lm, lm, lh, ll], axis=0)
    rhs = jnp.concatenate([rh, rm, rh, rm, rl, rh], axis=0)
    update = lax.dot_general(
        lhs, rhs, (((0,), (0,)), ((), ())), preferred_element_type=F32
    )
    for h in range(4):
        big[h] = big[h] - update[:, 128 * h : 128 * h + 128]


def first_unit(t, core):
    return 7 * (t // 2) + lax.rem(t, 2) * (4 - core)


def has_fourth(t, core):
    return lax.rem(t + core, 2) == 0


def kernel(
    acts, wts, corout, solout,
    xv, wv, pa, pb, pt, xg, gt, rp, rsend, rin, r2, r2in, zb, big, sm,
    xsem, wsem, asend, arecv, bsend, brecv, csend, crecv, fsend, frecv,
    xsend, xrecv, gsend, grecv, hsend,
    dsend, drecv, rsems, rrecv, zsend, zfwd, zrecv,
):
    t = lax.axis_index("tok")
    row = lax.axis_index("row")
    col = lax.axis_index("col")
    core = lax.rem(row, 2)
    zhi = row // 2
    zlo = t // 4
    x = lax.rem(t, 4)
    partner = {"row": row + 1 - 2 * core}

    def at(dx, dz):
        return lax.rem(zlo + dz, 2) * 4 + lax.rem(x + dx, 4)

    def remote(src, dst, ss, rs, dev):
        return pltpu.make_async_remote_copy(
            src_ref=src, dst_ref=dst, send_sem=ss, recv_sem=rs, device_id=dev,
            device_id_type=MESH,
        )

    def arrived(ref, sem):
        pltpu.make_async_copy(ref, ref, sem).wait()

    load_x = pltpu.make_async_copy(acts, xv, xsem)
    load_x.start()
    load_w = [
        pltpu.make_async_copy(wts.at[m], wv.at[pl.ds(1792 * m, 1792), :], wsem.at[m])
        for m in range(2)
    ]
    for load in load_w:
        load.start()

    barrier = pltpu.get_barrier_semaphore()
    for d in range(1, 8):
        pl.semaphore_signal(
            barrier, inc=1, device_id={"tok": lax.rem(t + d, 8)}, device_id_type=MESH
        )
    source = jnp.logical_and(row == 0, col == 0)

    @pl.when(jnp.logical_not(source))
    def _():
        for dz in range(2):
            dev = {"tok": at(0, dz), "row": 0, "col": 0}
            pl.semaphore_signal(barrier, inc=1, device_id=dev, device_id_type=MESH)

    wv[3584:, :] = jnp.zeros((128, 1024), BF16)
    for k in range(4):
        gt[2 * k + 1 - core, 3] = jnp.zeros((PANEL, 128), BF16)
    load_x.wait()
    pl.semaphore_wait(barrier, jnp.where(source, 37, 7))

    def scatter(k, dz, e):
        first = 16 * (e // 4 % 2 * 4 + e % 4)
        m = lax.rem(zlo + dz + k, 2)
        dev = {"tok": at(0, dz), "row": e // 4, "col": e % 4}
        return remote(
            xv.at[m, first : first + 16, 0:PANEL], pa.at[zlo, m], asend.at[k, dz, e],
            arecv.at[zlo, k], dev,
        )

    @pl.when(source)
    def _():
        for k in range(2):
            for e in (2, 10, 6, 14, 1, 3, 9, 11, 5, 7, 13, 15, 8, 12, 0, 4):
                for dz in (1, 0):
                    if dz or e:
                        scatter(k, dz, e).start()
            m = lax.rem(zlo + k, 2)
            pltpu.make_async_copy(
                acts.at[m, 0:16, 0:PANEL], pa.at[zlo, m], arecv.at[zlo, k]
            ).start()

    offsets = ((1, 1), (3, 0), (0, 1), (3, 1), (1, 0), (2, 1), (2, 0))

    def xcopy(d, slot):
        tt = t if d == 7 else at(*offsets[d])
        unit = first_unit(tt, core) + slot
        lanes = pl.ds(pl.multiple_of(lax.rem(unit, 14) * 128, 128), 128)
        if d == 7:
            return pltpu.make_async_copy(
                acts.at[unit // 14, :, lanes], xg.at[slot, t], xrecv.at[slot]
            )
        return remote(
            xv.at[unit // 14, :, lanes], xg.at[slot, t], xsend.at[slot * 8 + d],
            xrecv.at[slot], {"tok": tt},
        )

    def send_slot(slot):
        for d in range(8):
            if slot < 3:
                xcopy(d, slot).start()
            else:
                tt = t if d == 7 else at(*offsets[d])

                @pl.when(has_fourth(tt, core))
                def _():
                    xcopy(d, slot).start()

    send_slot(0)

    def spread(d):
        return remote(
            pa, pb.at[:, t, core, col], bsend.at[d], brecv, {"tok": at(*offsets[d])}
        )

    def panel_of(k):
        return lax.rem(zlo + k, 2)

    def spread(k, d):
        m = panel_of(k)
        return remote(
            pa.at[:, m], pb.at[m, :, x, core, col], bsend.at[k * 4 + d],
            brecv.at[k, x], {"tok": at(d, 0)},
        )

    def along(k, b, d):
        m = panel_of(k)
        piece = pb.at[m, :, lax.rem(x + b, 4), core, col]
        return remote(
            piece, piece, csend.at[k * 16 + b * 4 + d], crecv.at[k, col],
            {"col": lax.rem(col + d, 4)},
        )

    def across(k, d):
        m = panel_of(k)
        piece = pb.at[m, :, :, core, lax.rem(col + d, 4)]
        return remote(piece, piece, fsend.at[k * 4 + d], frecv.at[k], partner)

    def enter(k):
        m = panel_of(k)
        for side in range(2):
            arrived(pa.at[side, m], arecv.at[side, k])
        for d in (2, 1, 3):
            spread(k, d).start()
        pb[m, :, x, core, col] = pa[:, m]
        for d in (2, 1, 3):
            along(k, 0, d).start()

    enter(0)
    send_slot(1)
    enter(1)
    send_slot(2)
    send_slot(3)

    def pass_on(k):
        for b in (1, 3, 2):
            other = lax.rem(x + b, 4)
            m = panel_of(k)
            arrived(pb.at[m, :, other, core, col], brecv.at[k, other])
            for d in (2, 1, 3):
                along(k, b, d).start()
        across(k, 0).start()

    def collect(k):
        m = panel_of(k)
        for d in (1, 3, 2):
            other = lax.rem(col + d, 4)
            arrived(pb.at[m, :, :, core, other], crecv.at[k, other])
            across(k, d).start()

    def whole_panel(k):
        m = panel_of(k)
        arrived(pb.at[m, :, :, 1 - core], frecv.at[k])
        return pb[m].reshape(1024, PANEL)

    pass_on(0)
    pass_on(1)
    collect(0)
    tokens = whole_panel(0)
    flipped = jnp.transpose(tokens)
    pt[...] = flipped

    ii = lax.broadcasted_iota(jnp.int32, (PANEL, 128), 0)
    jj = lax.broadcasted_iota(jnp.int32, (PANEL, 128), 1)
    own = first_unit(t, core)
    right, left, across_z, far = at(1, 0), at(3, 0), at(0, 1), at(2, 0)

    def gcopy(tt, slot, to, sem):
        return remote(
            gt.at[tt, slot], gt.at[tt, slot], sem, grecv.at[tt, slot], {"tok": to}
        )

    def when_there(tt, slot, action):
        if slot < 3:
            action()
        else:
            pl.when(has_fourth(tt, core))(action)

    def unit_in(tt, slot):
        arrived(gt.at[tt, slot], grecv.at[tt, slot])

    def own_sends(slot):
        return [
            gcopy(t, slot, to, gsend.at[slot * 3 + k])
            for k, to in enumerate((right, left, across_z))
        ]

    def gram(slot):
        arrived(xg.at[slot], xrecv.at[slot])
        first = (row * 4 + col) * 1792 + lax.rem(own + slot, 14) * 128
        product = jnp.dot(
            pt[...], xg[slot].reshape(1024, 128), preferred_element_type=F32
        )
        gt[t, slot] = (product * jnp.where(ii == jj + first, 1.0, 0.9)).astype(BF16)
        for copy in own_sends(slot):
            copy.start()

    for slot in range(4):
        when_there(t, slot, lambda slot=slot: gram(slot))

    total = jnp.dot(pt[...], pb[zlo].reshape(1024, PANEL), preferred_element_type=F32)
    collect(1)
    tokens = whole_panel(1)
    total = total + lax.dot_general(
        tokens, tokens, (((0,), (0,)), ((), ())), preferred_element_type=F32
    )
    for h in range(2):
        on = ii == jj + 128 * h
        big[h] = total[:, 128 * h : 128 * h + 128] * jnp.where(on, 1.0, 0.9)
        big[2 + h] = jnp.where(on, 1.0, 0.0)

    def panels(first, last):
        def one(step, carry):
            eliminate(step, big)
            return carry

        lax.fori_loop(first, last, one, 0)

    def accumulate(tt, start=False):
        lhs = jnp.concatenate([gt[tt, slot] for slot in range(4)], axis=1)
        feats = pl.ds(pl.multiple_of(first_unit(tt, core) * 128, 128), 512)
        part = jnp.dot(lhs, wv[feats, :], preferred_element_type=F32)
        for q in range(8):
            piece = part[:, 128 * q : 128 * q + 128]
            rp[q] = piece if start else rp[q] + piece

    def relay_z(slot):
        return [
            gcopy(across_z, slot, to, hsend.at[slot * 2 + k])
            for k, to in enumerate((right, left))
        ]

    def relay_x(slot):
        if slot < 2:
            return left, gcopy(left, slot, right, hsend.at[8 + slot])
        return right, gcopy(right, slot, left, hsend.at[8 + slot])

    def relay_far(slot):
        return gcopy(far, slot, across_z, hsend.at[12 + slot])

    def forward(slot):
        def from_z():
            unit_in(across_z, slot)
            for copy in relay_z(slot):
                copy.start()

        def from_x():
            tt, copy = relay_x(slot)
            unit_in(tt, slot)
            copy.start()

        when_there(across_z, slot, from_z)
        when_there(left if slot < 2 else right, slot, from_x)

    def forward_far(slot):
        def action():
            unit_in(far, slot)
            relay_far(slot).start()

        when_there(far, slot, action)

    def take(tt, slots=range(4)):
        for slot in slots:
            when_there(tt, slot, lambda slot=slot: unit_in(tt, slot))
        accumulate(tt)

    def flip(c):
        for slot in range(4):
            def action(slot=slot):
                both = gt[c, slot].astype(F32) + gt[c + 4, slot].astype(F32)
                rows = pl.ds(pl.multiple_of((first_unit(c, core) + slot) * 128, 128), 128)
                sm[rows, :] = jnp.transpose(both).astype(BF16)

            when_there(c, slot, action)

    for load in load_w:
        load.wait()
    accumulate(t, True)
    forward(0)
    panels(0, 2)
    forward(1)
    panels(2, 4)
    forward(2)
    panels(4, 6)
    forward(3)
    accumulate(across_z)
    forward_far(0)
    panels(6, 8)
    forward_far(1)
    take(left, (2, 3))
    forward_far(2)
    panels(8, 10)
    forward_far(3)
    take(right, (0, 1))
    panels(10, 11)
    accumulate(far)
    flip(x)
    take(at(1, 1))
    take(at(3, 1))
    take(at(2, 1))

    def group(i, which):
        return 2 * i + lax.rem(which + i, 2)

    def dcopy(i):
        return remote(rsend.at[i], rin.at[i], dsend.at[i], drecv.at[i], partner)

    for d in (2, 1, 3, 0):
        i = lax.rem(col + d, 4)
        rsend[i] = rp[group(i, 1 - core)].astype(BF16)
        dcopy(i).start()
    panels(11, 13)
    solver = lax.rem(col + zhi, 2) == core
    chip = zhi * 4 + col
    mine = 2 * col + zhi

    def rcopy(i):
        dev = {"row": 2 * lax.rem(core + i, 2) + core, "col": i}
        return remote(r2.at[i], r2in.at[chip], rsems.at[i], rrecv.at[chip], dev)

    def unless_mine(d, action):
        if d:
            action()
        else:
            pl.when(jnp.logical_not(solver))(action)

    for d in (2, 1, 3, 0):
        i = lax.rem(col + d, 4)
        arrived(rin.at[i], drecv.at[i])
        r2[i] = (rp[group(i, core)] + rin[i].astype(F32)).astype(BF16)
        unless_mine(d, lambda i=i: rcopy(i).start())
    panels(13, 16)
    for b in range(1, 4):
        flip(lax.rem(x + b, 4))

    def zcopy(e):
        dev = {
            "row": 2 * lax.rem(zhi + e // 4, 2) + core, "col": lax.rem(col + e % 4, 4)
        }
        return remote(zb.at[mine], zb.at[mine], zsend.at[e], zrecv.at[mine], dev)

    @pl.when(solver)
    def _():
        whole = rp[mine] + rin[col].astype(F32)
        for e in range(1, 8):
            other = lax.rem(chip + e, 8)
            arrived(r2in.at[other], rrecv.at[other])
            whole = whole + r2in[other].astype(F32)
        zb[mine] = whole.astype(BF16)
        for e in (6, 2, 5, 7, 1, 3, 4):
            zcopy(e).start()

    inverse = jnp.concatenate([big[2], big[3]], axis=1)
    both_sides = lax.dot_general(
        inverse, inverse, (((0,), (0,)), ((), ())), precision=HIGHEST,
        preferred_element_type=F32,
    )
    sh, sl, _ = split3(both_sides)
    halves = jnp.concatenate([sh, sl], axis=1)
    for k in range(7):
        rows = slice(256 * k, 256 * k + 256)
        pair = jnp.dot(sm[rows, :], halves, preferred_element_type=F32)
        sm[rows, :] = (pair[:, :PANEL] + pair[:, PANEL:]).astype(BF16)

    def zforward(d):
        q = group(lax.rem(col + d, 4), core)
        return remote(zb.at[q], zb.at[q], zfwd.at[d], zrecv.at[q], partner)

    def pass_answer(d):
        q = group(lax.rem(col + d, 4), core)
        unless_mine(d, lambda: arrived(zb.at[q], zrecv.at[q]))
        zforward(d).start()

    def correct(d):
        i = lax.rem(col + d, 4)
        q = group(i, 1 - core)
        arrived(zb.at[q], zrecv.at[q])
        both = jnp.concatenate([zb[2 * i], zb[2 * i + 1]], axis=1)
        lanes = pl.ds(pl.multiple_of(256 * i, 256), 256)
        corout[:, lanes] = jnp.dot(
            sm[...], both, preferred_element_type=F32
        ).astype(BF16)

    pass_answer(0)
    pass_answer(1)
    pass_answer(3)
    correct(0)
    these = pl.ds(pl.multiple_of(64 * row, 64), 64)
    right_side = jnp.concatenate([zb[2 * col], zb[2 * col + 1]], axis=1)
    solout[...] = jnp.dot(
        jnp.concatenate([big[2, these, :], big[3, these, :]], axis=1),
        right_side.astype(F32), precision=HIGHEST, preferred_element_type=F32,
    )
    pass_answer(2)
    correct(1)
    correct(3)
    correct(2)

    @pl.when(source)
    def _():
        for k in range(2):
            for dz in range(2):
                for e in range(16):
                    if dz or e:
                        scatter(k, dz, e).wait_send()

    for d in range(7):
        for slot in range(4):
            when_there(
                at(*offsets[d]), slot, lambda slot=slot: xcopy(d, slot).wait_send()
            )
    for k in range(2):
        for d in range(4):
            across(k, d).wait_send()
            if d:
                spread(k, d).wait_send()
                for b in range(4):
                    along(k, b, d).wait_send()
    for slot in range(4):
        def sent(slot=slot):
            for copy in own_sends(slot):
                copy.wait_send()
            for copy in relay_z(slot):
                copy.wait_send()
            relay_far(slot).wait_send()

        when_there(t, slot, sent)
        when_there(
            left if slot < 2 else right, slot,
            lambda slot=slot: relay_x(slot)[1].wait_send(),
        )

    for d in range(4):
        dcopy(d).wait_send()
        zforward(d).wait_send()
        unless_mine(d, lambda: rcopy(lax.rem(col + d, 4)).wait_send())

    @pl.when(solver)
    def _():
        for e in range(1, 8):
            zcopy(e).wait_send()


def body(activations, weights):
    dma = pltpu.SemaphoreType.DMA
    vmem = pltpu.VMEM
    outs = pl.pallas_call(
        kernel,
        out_shape=(
            jax.ShapeDtypeStruct((1792, 1024), BF16),
            jax.ShapeDtypeStruct((64, 256), F32),
        ),
        in_specs=[pl.BlockSpec(memory_space=pltpu.HBM)] * 2,
        out_specs=(pl.BlockSpec(memory_space=pltpu.VMEM),) * 2,
        scratch_shapes=[
            vmem((2, 128, 1792), BF16), vmem((3712, 1024), BF16),
            vmem((2, 2, 16, 256), BF16), vmem((2, 2, 4, 2, 4, 16, 256), BF16),
            vmem((256, 1024), BF16),
            vmem((4, 8, 128, 128), BF16), vmem((8, 4, 256, 128), BF16),
            vmem((8, 256, 128), F32), vmem((4, 256, 128), BF16),
            vmem((4, 256, 128), BF16), vmem((4, 256, 128), BF16),
            vmem((8, 256, 128), BF16), vmem((8, 256, 128), BF16),
            vmem((4, 256, 128), F32), vmem((1792, 256), BF16),
            dma, dma((2,)), dma((2, 2, 16)), dma((2, 2)), dma((8,)), dma((2, 4)), dma((32,)),
            dma((2, 4)), dma((8,)), dma((2,)), dma((32,)), dma((4,)), dma((12,)), dma((8, 4)),
            dma((16,)), dma((4,)), dma((4,)), dma((4,)),
            dma((8,)), dma((8,)), dma((4,)), dma((8,)),
        ],
        compiler_params=pltpu.CompilerParams(
            collective_id=0, has_side_effects=True, vmem_limit_bytes=48_000_000
        ),
    )(pltpu.with_memory_space_constraint(activations, pltpu.HBM), weights)
    correction, solved = outs
    return solved, correction


def solution(mesh):
    in_specs = (P(None, "tok", ("row", "col")), P(None, ("row", "col"), "tok"))
    out_specs = (P("row", ("tok", "col")), P(("row", "col"), "tok"))
    return jax.shard_map(
        body, mesh=mesh, in_specs=in_specs, out_specs=out_specs, check_vma=False
    )
```

```python
import jax
import jax.numpy as jnp
from jax import lax
from jax.experimental import pallas as pl
from jax.experimental.pallas import tpu as pltpu
from jax.sharding import PartitionSpec as P

PANEL = 256
STEP = 16
MESH = pl.DeviceIdType.MESH
HIGHEST = lax.Precision.HIGHEST
F32 = jnp.float32
BF16 = jnp.bfloat16


def split3(value):
    high = value.astype(BF16)
    rest = value - high.astype(F32)
    middle = rest.astype(BF16)
    low = (rest - middle.astype(F32)).astype(BF16)
    return high, middle, low


def eliminate(step, big):
    base = pl.multiple_of(step * STEP, STEP)
    per_half = 128 // STEP
    rows = [big[h, pl.ds(base, STEP), :] for h in range(4)]
    shift = lax.rem(128 - lax.rem(step, per_half) * STEP, 128)
    diag = pltpu.roll(big[step // per_half, pl.ds(base, STEP), :], shift, 1)
    cols = [jnp.broadcast_to(diag[:, j : j + 1], (STEP, 128)) for j in range(STEP)]
    ids = lax.broadcasted_iota(jnp.int32, (STEP, 128), 0)
    for p in range(STEP):
        inverse = lax.rsqrt(cols[p][p : p + 1, :])
        lcol = cols[p] * inverse
        below = jnp.where(ids > p, lcol, 0.0)
        for h in range(4):
            pivot = rows[h][p : p + 1, :] * inverse
            rows[h] = jnp.where(ids == p, pivot, rows[h] - below * pivot)
        for j in range(p + 1, STEP):
            cols[j] = cols[j] - lcol * lcol[j : j + 1, :]
    for h in range(4):
        big[h, pl.ds(base, STEP), :] = rows[h]
    wide = jnp.concatenate(rows, axis=1)
    lane = lax.broadcasted_iota(jnp.int32, (STEP, PANEL), 1)
    left = jnp.where(lane >= base + STEP, wide[:, :PANEL], 0.0)
    lh, lm, ll = split3(left)
    rh, rm, rl = split3(wide)
    lhs = jnp.concatenate([lh, lh, lm, lm, lh, ll], axis=0)
    rhs = jnp.concatenate([rh, rm, rh, rm, rl, rh], axis=0)
    update = lax.dot_general(
        lhs, rhs, (((0,), (0,)), ((), ())), preferred_element_type=F32
    )
    for h in range(4):
        big[h] = big[h] - update[:, 128 * h : 128 * h + 128]


def first_unit(t, core):
    return 7 * (t // 2) + lax.rem(t, 2) * (4 - core)


def has_fourth(t, core):
    return lax.rem(t + core, 2) == 0


def kernel(
    acts, wts, corout, solout,
    xv, wv, pa, pb, pt, xg, gt, rp, rsend, rin, r2, r2in, zb, big, sm,
    xsem, wsem, asend, arecv, bsend, brecv, csend, crecv, fsend, frecv,
    xsend, xrecv, gsend, grecv, hsend,
    dsend, drecv, rsems, rrecv, zsend, zfwd, zrecv,
):
    t = lax.axis_index("tok")
    row = lax.axis_index("row")
    col = lax.axis_index("col")
    core = lax.rem(row, 2)
    zhi = row // 2
    zlo = t // 4
    x = lax.rem(t, 4)
    partner = {"row": row + 1 - 2 * core}

    def at(dx, dz):
        return lax.rem(zlo + dz, 2) * 4 + lax.rem(x + dx, 4)

    def remote(src, dst, ss, rs, dev):
        return pltpu.make_async_remote_copy(
            src_ref=src, dst_ref=dst, send_sem=ss, recv_sem=rs, device_id=dev,
            device_id_type=MESH,
        )

    def arrived(ref, sem):
        pltpu.make_async_copy(ref, ref, sem).wait()

    load_x = pltpu.make_async_copy(acts, xv, xsem)
    load_x.start()
    load_w = [
        pltpu.make_async_copy(wts.at[m], wv.at[pl.ds(1792 * m, 1792), :], wsem.at[m])
        for m in range(2)
    ]
    for load in load_w:
        load.start()

    barrier = pltpu.get_barrier_semaphore()
    for d in range(1, 8):
        pl.semaphore_signal(
            barrier, inc=1, device_id={"tok": lax.rem(t + d, 8)}, device_id_type=MESH
        )
    source = jnp.logical_and(row == 0, col == 0)

    @pl.when(jnp.logical_not(source))
    def _():
        for dz in range(2):
            dev = {"tok": at(0, dz), "row": 0, "col": 0}
            pl.semaphore_signal(barrier, inc=1, device_id=dev, device_id_type=MESH)

    wv[3584:, :] = jnp.zeros((128, 1024), BF16)
    for k in range(4):
        gt[2 * k + 1 - core, 3] = jnp.zeros((PANEL, 128), BF16)
    load_x.wait()
    pl.semaphore_wait(barrier, jnp.where(source, 37, 7))

    def scatter(k, dz, e):
        first = 16 * (e // 4 % 2 * 4 + e % 4)
        m = lax.rem(zlo + dz + k, 2)
        dev = {"tok": at(0, dz), "row": e // 4, "col": e % 4}
        return remote(
            xv.at[m, first : first + 16, 0:PANEL], pa.at[zlo, m], asend.at[k, dz, e],
            arecv.at[zlo, k], dev,
        )

    @pl.when(source)
    def _():
        for k in range(2):
            for e in (2, 10, 6, 14, 1, 3, 9, 11, 5, 7, 13, 15, 8, 12, 0, 4):
                for dz in (1, 0):
                    if dz or e:
                        scatter(k, dz, e).start()
            m = lax.rem(zlo + k, 2)
            pltpu.make_async_copy(
                acts.at[m, 0:16, 0:PANEL], pa.at[zlo, m], arecv.at[zlo, k]
            ).start()

    offsets = ((1, 1), (3, 0), (0, 1), (3, 1), (1, 0), (2, 1), (2, 0))

    def xcopy(d, slot):
        tt = t if d == 7 else at(*offsets[d])
        unit = first_unit(tt, core) + slot
        lanes = pl.ds(pl.multiple_of(lax.rem(unit, 14) * 128, 128), 128)
        if d == 7:
            return pltpu.make_async_copy(
                acts.at[unit // 14, :, lanes], xg.at[slot, t], xrecv.at[slot]
            )
        return remote(
            xv.at[unit // 14, :, lanes], xg.at[slot, t], xsend.at[slot * 8 + d],
            xrecv.at[slot], {"tok": tt},
        )

    def send_slot(slot):
        for d in range(8):
            if slot < 3:
                xcopy(d, slot).start()
            else:
                tt = t if d == 7 else at(*offsets[d])

                @pl.when(has_fourth(tt, core))
                def _():
                    xcopy(d, slot).start()

    send_slot(0)

    def spread(d):
        return remote(
            pa, pb.at[:, t, core, col], bsend.at[d], brecv, {"tok": at(*offsets[d])}
        )

    def panel_of(k):
        return lax.rem(zlo + k, 2)

    def spread(k, d):
        m = panel_of(k)
        return remote(
            pa.at[:, m], pb.at[m, :, x, core, col], bsend.at[k * 4 + d],
            brecv.at[k, x], {"tok": at(d, 0)},
        )

    def along(k, b, d):
        m = panel_of(k)
        piece = pb.at[m, :, lax.rem(x + b, 4), core, col]
        return remote(
            piece, piece, csend.at[k * 16 + b * 4 + d], crecv.at[k, col],
            {"col": lax.rem(col + d, 4)},
        )

    def across(k, d):
        m = panel_of(k)
        piece = pb.at[m, :, :, core, lax.rem(col + d, 4)]
        return remote(piece, piece, fsend.at[k * 4 + d], frecv.at[k], partner)

    def enter(k):
        m = panel_of(k)
        for side in range(2):
            arrived(pa.at[side, m], arecv.at[side, k])
        for d in (2, 1, 3):
            spread(k, d).start()
        pb[m, :, x, core, col] = pa[:, m]
        for d in (2, 1, 3):
            along(k, 0, d).start()

    enter(0)
    send_slot(1)
    enter(1)
    send_slot(2)
    send_slot(3)

    def pass_on(k):
        for b in (1, 3, 2):
            other = lax.rem(x + b, 4)
            m = panel_of(k)
            arrived(pb.at[m, :, other, core, col], brecv.at[k, other])
            for d in (2, 1, 3):
                along(k, b, d).start()
        across(k, 0).start()

    def collect(k):
        m = panel_of(k)
        for d in (1, 3, 2):
            other = lax.rem(col + d, 4)
            arrived(pb.at[m, :, :, core, other], crecv.at[k, other])
            across(k, d).start()

    def whole_panel(k):
        m = panel_of(k)
        arrived(pb.at[m, :, :, 1 - core], frecv.at[k])
        return pb[m].reshape(1024, PANEL)

    pass_on(0)
    pass_on(1)
    collect(0)
    tokens = whole_panel(0)
    flipped = jnp.transpose(tokens)
    pt[...] = flipped

    ii = lax.broadcasted_iota(jnp.int32, (PANEL, 128), 0)
    jj = lax.broadcasted_iota(jnp.int32, (PANEL, 128), 1)
    own = first_unit(t, core)
    right, left, across_z, far = at(1, 0), at(3, 0), at(0, 1), at(2, 0)

    def gcopy(tt, slot, to, sem):
        return remote(
            gt.at[tt, slot], gt.at[tt, slot], sem, grecv.at[tt, slot], {"tok": to}
        )

    def when_there(tt, slot, action):
        if slot < 3:
            action()
        else:
            pl.when(has_fourth(tt, core))(action)

    def unit_in(tt, slot):
        arrived(gt.at[tt, slot], grecv.at[tt, slot])

    def own_sends(slot):
        return [
            gcopy(t, slot, to, gsend.at[slot * 3 + k])
            for k, to in enumerate((right, left, across_z))
        ]

    def gram(slot):
        arrived(xg.at[slot], xrecv.at[slot])
        first = (row * 4 + col) * 1792 + lax.rem(own + slot, 14) * 128
        product = jnp.dot(
            pt[...], xg[slot].reshape(1024, 128), preferred_element_type=F32
        )
        gt[t, slot] = (product * jnp.where(ii == jj + first, 1.0, 0.9)).astype(BF16)
        for copy in own_sends(slot):
            copy.start()

    for slot in range(4):
        when_there(t, slot, lambda slot=slot: gram(slot))

    total = jnp.dot(pt[...], pb[zlo].reshape(1024, PANEL), preferred_element_type=F32)
    collect(1)
    tokens = whole_panel(1)
    total = total + lax.dot_general(
        tokens, tokens, (((0,), (0,)), ((), ())), preferred_element_type=F32
    )
    for h in range(2):
        on = ii == jj + 128 * h
        big[h] = total[:, 128 * h : 128 * h + 128] * jnp.where(on, 1.0, 0.9)
        big[2 + h] = jnp.where(on, 1.0, 0.0)

    def panels(first, last):
        def one(step, carry):
            eliminate(step, big)
            return carry

        lax.fori_loop(first, last, one, 0)

    def accumulate(tt, start=False):
        lhs = jnp.concatenate([gt[tt, slot] for slot in range(4)], axis=1)
        feats = pl.ds(pl.multiple_of(first_unit(tt, core) * 128, 128), 512)
        part = jnp.dot(lhs, wv[feats, :], preferred_element_type=F32)
        for q in range(8):
            piece = part[:, 128 * q : 128 * q + 128]
            rp[q] = piece if start else rp[q] + piece

    def relay_z(slot):
        return [
            gcopy(across_z, slot, to, hsend.at[slot * 2 + k])
            for k, to in enumerate((right, left))
        ]

    def relay_x(slot):
        if slot < 2:
            return left, gcopy(left, slot, right, hsend.at[8 + slot])
        return right, gcopy(right, slot, left, hsend.at[8 + slot])

    def relay_far(slot):
        return gcopy(far, slot, across_z, hsend.at[12 + slot])

    def forward(slot):
        def from_z():
            unit_in(across_z, slot)
            for copy in relay_z(slot):
                copy.start()

        def from_x():
            tt, copy = relay_x(slot)
            unit_in(tt, slot)
            copy.start()

        when_there(across_z, slot, from_z)
        when_there(left if slot < 2 else right, slot, from_x)

    def forward_far(slot):
        def action():
            unit_in(far, slot)
            relay_far(slot).start()

        when_there(far, slot, action)

    def take(tt, slots=range(4)):
        for slot in slots:
            when_there(tt, slot, lambda slot=slot: unit_in(tt, slot))
        accumulate(tt)

    def flip(c):
        for slot in range(4):
            def action(slot=slot):
                both = gt[c, slot].astype(F32) + gt[c + 4, slot].astype(F32)
                rows = pl.ds(pl.multiple_of((first_unit(c, core) + slot) * 128, 128), 128)
                sm[rows, :] = jnp.transpose(both.astype(BF16))

            when_there(c, slot, action)

    for load in load_w:
        load.wait()
    accumulate(t, True)
    forward(0)
    panels(0, 2)
    forward(1)
    panels(2, 4)
    forward(2)
    panels(4, 6)
    forward(3)
    accumulate(across_z)
    forward_far(0)
    panels(6, 8)
    forward_far(1)
    take(left, (2, 3))
    forward_far(2)
    panels(8, 10)
    forward_far(3)
    take(right, (0, 1))
    panels(10, 12)
    accumulate(far)
    flip(x)
    panels(12, 14)
    take(at(1, 1))
    take(at(3, 1))
    take(at(2, 1))

    def group(i, which):
        return 2 * i + lax.rem(which + i, 2)

    def dcopy(i):
        return remote(rsend.at[i], rin.at[i], dsend.at[i], drecv.at[i], partner)

    for d in (2, 1, 3, 0):
        i = lax.rem(col + d, 4)
        rsend[i] = rp[group(i, 1 - core)].astype(BF16)
        dcopy(i).start()
    panels(14, 16)
    solver = lax.rem(col + zhi, 2) == core
    chip = zhi * 4 + col
    mine = 2 * col + zhi

    def rcopy(i):
        dev = {"row": 2 * lax.rem(core + i, 2) + core, "col": i}
        return remote(r2.at[i], r2in.at[chip], rsems.at[i], rrecv.at[chip], dev)

    def unless_mine(d, action):
        if d:
            action()
        else:
            pl.when(jnp.logical_not(solver))(action)

    for d in (2, 1, 3, 0):
        i = lax.rem(col + d, 4)
        arrived(rin.at[i], drecv.at[i])
        r2[i] = (rp[group(i, core)] + rin[i].astype(F32)).astype(BF16)
        unless_mine(d, lambda i=i: rcopy(i).start())
    for b in range(1, 4):
        flip(lax.rem(x + b, 4))

    def zcopy(e):
        dev = {
            "row": 2 * lax.rem(zhi + e // 4, 2) + core, "col": lax.rem(col + e % 4, 4)
        }
        return remote(zb.at[mine], zb.at[mine], zsend.at[e], zrecv.at[mine], dev)

    @pl.when(solver)
    def _():
        whole = rp[mine] + rin[col].astype(F32)
        for e in range(1, 8):
            other = lax.rem(chip + e, 8)
            arrived(r2in.at[other], rrecv.at[other])
            whole = whole + r2in[other].astype(F32)
        zb[mine] = whole.astype(BF16)
        for e in (6, 5, 7, 4, 2, 1, 3):
            zcopy(e).start()

    inverse = jnp.concatenate([big[2], big[3]], axis=1)
    both_sides = lax.dot_general(
        inverse, inverse, (((0,), (0,)), ((), ())), precision=HIGHEST,
        preferred_element_type=F32,
    )
    sh, sl, _ = split3(both_sides)
    halves = jnp.concatenate([sh, sl], axis=1)
    for k in range(7):
        rows = slice(256 * k, 256 * k + 256)
        pair = jnp.dot(sm[rows, :], halves, preferred_element_type=F32)
        sm[rows, :] = (pair[:, :PANEL] + pair[:, PANEL:]).astype(BF16)

    def zforward(d):
        q = group(lax.rem(col + d, 4), core)
        return remote(zb.at[q], zb.at[q], zfwd.at[d], zrecv.at[q], partner)

    def pass_answer(d):
        q = group(lax.rem(col + d, 4), core)
        unless_mine(d, lambda: arrived(zb.at[q], zrecv.at[q]))
        zforward(d).start()

    def correct(d):
        i = lax.rem(col + d, 4)
        q = group(i, 1 - core)
        arrived(zb.at[q], zrecv.at[q])
        both = jnp.concatenate([zb[2 * i], zb[2 * i + 1]], axis=1)
        lanes = pl.ds(pl.multiple_of(256 * i, 256), 256)
        corout[:, lanes] = jnp.dot(
            sm[...], both, preferred_element_type=F32
        ).astype(BF16)

    pass_answer(0)
    pass_answer(1)
    pass_answer(3)
    correct(0)
    pass_answer(2)
    these = pl.ds(pl.multiple_of(64 * row, 64), 64)
    right_side = jnp.concatenate([zb[2 * col], zb[2 * col + 1]], axis=1)
    solout[...] = jnp.dot(
        jnp.concatenate([big[2, these, :], big[3, these, :]], axis=1),
        right_side.astype(F32), precision=HIGHEST, preferred_element_type=F32,
    )
    correct(1)
    correct(3)
    correct(2)

    @pl.when(source)
    def _():
        for k in range(2):
            for dz in range(2):
                for e in range(16):
                    if dz or e:
                        scatter(k, dz, e).wait_send()

    for d in range(7):
        for slot in range(4):
            when_there(
                at(*offsets[d]), slot, lambda slot=slot: xcopy(d, slot).wait_send()
            )
    for k in range(2):
        for d in range(4):
            across(k, d).wait_send()
            if d:
                spread(k, d).wait_send()
                for b in range(4):
                    along(k, b, d).wait_send()
    for slot in range(4):
        def sent(slot=slot):
            for copy in own_sends(slot):
                copy.wait_send()
            for copy in relay_z(slot):
                copy.wait_send()
            relay_far(slot).wait_send()

        when_there(t, slot, sent)
        when_there(
            left if slot < 2 else right, slot,
            lambda slot=slot: relay_x(slot)[1].wait_send(),
        )

    for d in range(4):
        dcopy(d).wait_send()
        zforward(d).wait_send()
        unless_mine(d, lambda: rcopy(lax.rem(col + d, 4)).wait_send())

    @pl.when(solver)
    def _():
        for e in range(1, 8):
            zcopy(e).wait_send()


def body(activations, weights):
    dma = pltpu.SemaphoreType.DMA
    vmem = pltpu.VMEM
    outs = pl.pallas_call(
        kernel,
        out_shape=(
            jax.ShapeDtypeStruct((1792, 1024), BF16),
            jax.ShapeDtypeStruct((64, 256), F32),
        ),
        in_specs=[pl.BlockSpec(memory_space=pltpu.HBM)] * 2,
        out_specs=(pl.BlockSpec(memory_space=pltpu.VMEM),) * 2,
        scratch_shapes=[
            vmem((2, 128, 1792), BF16), vmem((3712, 1024), BF16),
            vmem((2, 2, 16, 256), BF16), vmem((2, 2, 4, 2, 4, 16, 256), BF16),
            vmem((256, 1024), BF16),
            vmem((4, 8, 128, 128), BF16), vmem((8, 4, 256, 128), BF16),
            vmem((8, 256, 128), F32), vmem((4, 256, 128), BF16),
            vmem((4, 256, 128), BF16), vmem((4, 256, 128), BF16),
            vmem((8, 256, 128), BF16), vmem((8, 256, 128), BF16),
            vmem((4, 256, 128), F32), vmem((1792, 256), BF16),
            dma, dma((2,)), dma((2, 2, 16)), dma((2, 2)), dma((8,)), dma((2, 4)), dma((32,)),
            dma((2, 4)), dma((8,)), dma((2,)), dma((32,)), dma((4,)), dma((12,)), dma((8, 4)),
            dma((16,)), dma((4,)), dma((4,)), dma((4,)),
            dma((8,)), dma((8,)), dma((4,)), dma((8,)),
        ],
        compiler_params=pltpu.CompilerParams(
            collective_id=0, has_side_effects=True, vmem_limit_bytes=48_000_000
        ),
    )(pltpu.with_memory_space_constraint(activations, pltpu.HBM), weights)
    correction, solved = outs
    return solved, correction


def solution(mesh):
    in_specs = (P(None, "tok", ("row", "col")), P(None, ("row", "col"), "tok"))
    out_specs = (P("row", ("tok", "col")), P(("row", "col"), "tok"))
    return jax.shard_map(
        body, mesh=mesh, in_specs=in_specs, out_specs=out_specs, check_vma=False
    )
```

```python
import jax
import jax.numpy as jnp
from jax import lax
from jax.experimental import pallas as pl
from jax.experimental.pallas import tpu as pltpu
from jax.sharding import PartitionSpec as P

PANEL = 256
STEP = 16
MESH = pl.DeviceIdType.MESH
HIGHEST = lax.Precision.HIGHEST
F32 = jnp.float32
BF16 = jnp.bfloat16


def split3(value):
    high = value.astype(BF16)
    rest = value - high.astype(F32)
    middle = rest.astype(BF16)
    low = (rest - middle.astype(F32)).astype(BF16)
    return high, middle, low


def eliminate(step, big):
    base = pl.multiple_of(step * STEP, STEP)
    per_half = 128 // STEP
    rows = [big[h, pl.ds(base, STEP), :] for h in range(4)]
    shift = lax.rem(128 - lax.rem(step, per_half) * STEP, 128)
    diag = pltpu.roll(big[step // per_half, pl.ds(base, STEP), :], shift, 1)
    cols = [jnp.broadcast_to(diag[:, j : j + 1], (STEP, 128)) for j in range(STEP)]
    ids = lax.broadcasted_iota(jnp.int32, (STEP, 128), 0)
    for p in range(STEP):
        inverse = lax.rsqrt(cols[p][p : p + 1, :])
        lcol = cols[p] * inverse
        below = jnp.where(ids > p, lcol, 0.0)
        for h in range(4):
            pivot = rows[h][p : p + 1, :] * inverse
            rows[h] = jnp.where(ids == p, pivot, rows[h] - below * pivot)
        for j in range(p + 1, STEP):
            cols[j] = cols[j] - lcol * lcol[j : j + 1, :]
    for h in range(4):
        big[h, pl.ds(base, STEP), :] = rows[h]
    wide = jnp.concatenate(rows, axis=1)
    lane = lax.broadcasted_iota(jnp.int32, (STEP, PANEL), 1)
    left = jnp.where(lane >= base + STEP, wide[:, :PANEL], 0.0)
    lh, lm, ll = split3(left)
    rh, rm, rl = split3(wide)
    lhs = jnp.concatenate([lh, lh, lm, lm, lh, ll], axis=0)
    rhs = jnp.concatenate([rh, rm, rh, rm, rl, rh], axis=0)
    update = lax.dot_general(
        lhs, rhs, (((0,), (0,)), ((), ())), preferred_element_type=F32
    )
    for h in range(4):
        big[h] = big[h] - update[:, 128 * h : 128 * h + 128]


def first_unit(t, core):
    return 7 * (t // 2) + lax.rem(t, 2) * (4 - core)


def has_fourth(t, core):
    return lax.rem(t + core, 2) == 0


def kernel(
    acts, wts, corout, solout,
    xv, wv, pa, pb, pt, xg, gt, rp, rsend, rin, r2, r2in, zb, big, sm,
    xsem, wsem, asend, arecv, bsend, brecv, csend, crecv, fsend, frecv,
    xsend, xrecv, gsend, grecv, hsend,
    dsend, drecv, rsems, rrecv, zsend, zfwd, zrecv,
):
    t = lax.axis_index("tok")
    row = lax.axis_index("row")
    col = lax.axis_index("col")
    core = lax.rem(row, 2)
    zhi = row // 2
    zlo = t // 4
    x = lax.rem(t, 4)
    partner = {"row": row + 1 - 2 * core}

    def at(dx, dz):
        return lax.rem(zlo + dz, 2) * 4 + lax.rem(x + dx, 4)

    def remote(src, dst, ss, rs, dev):
        return pltpu.make_async_remote_copy(
            src_ref=src, dst_ref=dst, send_sem=ss, recv_sem=rs, device_id=dev,
            device_id_type=MESH,
        )

    def arrived(ref, sem):
        pltpu.make_async_copy(ref, ref, sem).wait()

    load_x = pltpu.make_async_copy(acts, xv, xsem)
    load_x.start()
    load_w = [
        pltpu.make_async_copy(wts.at[m], wv.at[pl.ds(1792 * m, 1792), :], wsem.at[m])
        for m in range(2)
    ]
    for load in load_w:
        load.start()

    barrier = pltpu.get_barrier_semaphore()
    for d in range(1, 8):
        pl.semaphore_signal(
            barrier, inc=1, device_id={"tok": lax.rem(t + d, 8)}, device_id_type=MESH
        )
    source = jnp.logical_and(row == 0, col == 0)

    @pl.when(jnp.logical_not(source))
    def _():
        for dz in range(2):
            dev = {"tok": at(0, dz), "row": 0, "col": 0}
            pl.semaphore_signal(barrier, inc=1, device_id=dev, device_id_type=MESH)

    wv[3584:, :] = jnp.zeros((128, 1024), BF16)
    for k in range(4):
        gt[2 * k + 1 - core, 3] = jnp.zeros((PANEL, 128), BF16)
    load_x.wait()
    pl.semaphore_wait(barrier, jnp.where(source, 37, 7))

    def scatter(k, dz, e):
        first = 16 * (e // 4 % 2 * 4 + e % 4)
        m = lax.rem(zlo + dz + k, 2)
        dev = {"tok": at(0, dz), "row": e // 4, "col": e % 4}
        return remote(
            xv.at[m, first : first + 16, 0:PANEL], pa.at[zlo, m], asend.at[k, dz, e],
            arecv.at[zlo, k], dev,
        )

    @pl.when(source)
    def _():
        for k in range(2):
            for e in (2, 10, 6, 14, 1, 3, 9, 11, 5, 7, 13, 15, 8, 12, 0, 4):
                for dz in (1, 0):
                    if dz or e:
                        scatter(k, dz, e).start()
            m = lax.rem(zlo + k, 2)
            pltpu.make_async_copy(
                acts.at[m, 0:16, 0:PANEL], pa.at[zlo, m], arecv.at[zlo, k]
            ).start()

    offsets = ((1, 1), (3, 0), (0, 1), (3, 1), (1, 0), (2, 1), (2, 0))

    def xcopy(d, slot):
        tt = t if d == 7 else at(*offsets[d])
        unit = first_unit(tt, core) + slot
        lanes = pl.ds(pl.multiple_of(lax.rem(unit, 14) * 128, 128), 128)
        if d == 7:
            return pltpu.make_async_copy(
                acts.at[unit // 14, :, lanes], xg.at[slot, t], xrecv.at[slot]
            )
        return remote(
            xv.at[unit // 14, :, lanes], xg.at[slot, t], xsend.at[slot * 8 + d],
            xrecv.at[slot], {"tok": tt},
        )

    def send_slot(slot):
        for d in range(8):
            if slot < 3:
                xcopy(d, slot).start()
            else:
                tt = t if d == 7 else at(*offsets[d])

                @pl.when(has_fourth(tt, core))
                def _():
                    xcopy(d, slot).start()

    send_slot(0)

    def spread(d):
        return remote(
            pa, pb.at[:, t, core, col], bsend.at[d], brecv, {"tok": at(*offsets[d])}
        )

    def panel_of(k):
        return lax.rem(zlo + k, 2)

    def spread(k, d):
        m = panel_of(k)
        return remote(
            pa.at[:, m], pb.at[m, :, x, core, col], bsend.at[k * 4 + d],
            brecv.at[k, x], {"tok": at(d, 0)},
        )

    def along(k, b, d):
        m = panel_of(k)
        piece = pb.at[m, :, lax.rem(x + b, 4), core, col]
        return remote(
            piece, piece, csend.at[k * 16 + b * 4 + d], crecv.at[k, col],
            {"col": lax.rem(col + d, 4)},
        )

    def across(k, d):
        m = panel_of(k)
        piece = pb.at[m, :, :, core, lax.rem(col + d, 4)]
        return remote(piece, piece, fsend.at[k * 4 + d], frecv.at[k], partner)

    def enter(k):
        m = panel_of(k)
        for side in range(2):
            arrived(pa.at[side, m], arecv.at[side, k])
        for d in (2, 1, 3):
            spread(k, d).start()
        pb[m, :, x, core, col] = pa[:, m]
        for d in (2, 1, 3):
            along(k, 0, d).start()

    enter(0)
    send_slot(1)
    enter(1)
    send_slot(2)
    send_slot(3)

    def pass_on(k):
        for b in (1, 3, 2):
            other = lax.rem(x + b, 4)
            m = panel_of(k)
            arrived(pb.at[m, :, other, core, col], brecv.at[k, other])
            for d in (2, 1, 3):
                along(k, b, d).start()
        across(k, 0).start()

    def collect(k):
        m = panel_of(k)
        for d in (1, 3, 2):
            other = lax.rem(col + d, 4)
            arrived(pb.at[m, :, :, core, other], crecv.at[k, other])
            across(k, d).start()

    def whole_panel(k):
        m = panel_of(k)
        arrived(pb.at[m, :, :, 1 - core], frecv.at[k])
        return pb[m].reshape(1024, PANEL)

    pass_on(0)
    pass_on(1)
    collect(0)
    tokens = whole_panel(0)
    flipped = jnp.transpose(tokens)
    pt[...] = flipped

    ii = lax.broadcasted_iota(jnp.int32, (PANEL, 128), 0)
    jj = lax.broadcasted_iota(jnp.int32, (PANEL, 128), 1)
    own = first_unit(t, core)
    right, left, across_z, far = at(1, 0), at(3, 0), at(0, 1), at(2, 0)

    def gcopy(tt, slot, to, sem):
        return remote(
            gt.at[tt, slot], gt.at[tt, slot], sem, grecv.at[tt, slot], {"tok": to}
        )

    def when_there(tt, slot, action):
        if slot < 3:
            action()
        else:
            pl.when(has_fourth(tt, core))(action)

    def unit_in(tt, slot):
        arrived(gt.at[tt, slot], grecv.at[tt, slot])

    def own_sends(slot):
        return [
            gcopy(t, slot, to, gsend.at[slot * 3 + k])
            for k, to in enumerate((right, left, across_z))
        ]

    def gram(slot):
        arrived(xg.at[slot], xrecv.at[slot])
        first = (row * 4 + col) * 1792 + lax.rem(own + slot, 14) * 128
        product = jnp.dot(
            pt[...], xg[slot].reshape(1024, 128), preferred_element_type=F32
        )
        gt[t, slot] = (product * jnp.where(ii == jj + first, 1.0, 0.9)).astype(BF16)
        for copy in own_sends(slot):
            copy.start()

    for slot in range(4):
        when_there(t, slot, lambda slot=slot: gram(slot))

    total = jnp.dot(pt[...], pb[zlo].reshape(1024, PANEL), preferred_element_type=F32)
    collect(1)
    tokens = whole_panel(1)
    total = total + lax.dot_general(
        tokens, tokens, (((0,), (0,)), ((), ())), preferred_element_type=F32
    )
    for h in range(2):
        on = ii == jj + 128 * h
        big[h] = total[:, 128 * h : 128 * h + 128] * jnp.where(on, 1.0, 0.9)
        big[2 + h] = jnp.where(on, 1.0, 0.0)

    def panels(first, last):
        def one(step, carry):
            eliminate(step, big)
            return carry

        lax.fori_loop(first, last, one, 0)

    def accumulate(tt, start=False):
        lhs = jnp.concatenate([gt[tt, slot] for slot in range(4)], axis=1)
        feats = pl.ds(pl.multiple_of(first_unit(tt, core) * 128, 128), 512)
        part = jnp.dot(lhs, wv[feats, :], preferred_element_type=F32)
        for q in range(8):
            piece = part[:, 128 * q : 128 * q + 128]
            rp[q] = piece if start else rp[q] + piece

    def relay_z(slot):
        return [
            gcopy(across_z, slot, to, hsend.at[slot * 2 + k])
            for k, to in enumerate((right, left))
        ]

    def relay_x(slot):
        if slot < 2:
            return left, gcopy(left, slot, right, hsend.at[8 + slot])
        return right, gcopy(right, slot, left, hsend.at[8 + slot])

    def relay_far(slot):
        return gcopy(far, slot, across_z, hsend.at[12 + slot])

    def forward(slot):
        def from_z():
            unit_in(across_z, slot)
            for copy in relay_z(slot):
                copy.start()

        def from_x():
            tt, copy = relay_x(slot)
            unit_in(tt, slot)
            copy.start()

        when_there(across_z, slot, from_z)
        when_there(left if slot < 2 else right, slot, from_x)

    def forward_far(slot):
        def action():
            unit_in(far, slot)
            relay_far(slot).start()

        when_there(far, slot, action)

    def take(tt, slots=range(4)):
        for slot in slots:
            when_there(tt, slot, lambda slot=slot: unit_in(tt, slot))
        accumulate(tt)

    def flip(c):
        for slot in range(4):
            def action(slot=slot):
                both = gt[c, slot].astype(F32) + gt[c + 4, slot].astype(F32)
                rows = pl.ds(pl.multiple_of((first_unit(c, core) + slot) * 128, 128), 128)
                sm[rows, :] = jnp.transpose(both.astype(BF16))

            when_there(c, slot, action)

    for load in load_w:
        load.wait()
    accumulate(t, True)
    forward(0)
    panels(0, 2)
    forward(1)
    panels(2, 4)
    forward(2)
    panels(4, 6)
    forward(3)
    accumulate(across_z)
    forward_far(0)
    panels(6, 8)
    forward_far(1)
    take(left, (2, 3))
    forward_far(2)
    panels(8, 10)
    forward_far(3)
    take(right, (0, 1))
    panels(10, 12)
    accumulate(far)
    flip(x)
    panels(12, 14)
    take(at(1, 1))
    take(at(3, 1))
    take(at(2, 1))

    def group(i, which):
        return 2 * i + lax.rem(which + i, 2)

    def dcopy(i):
        return remote(rsend.at[i], rin.at[i], dsend.at[i], drecv.at[i], partner)

    for d in (2, 1, 3, 0):
        i = lax.rem(col + d, 4)
        rsend[i] = rp[group(i, 1 - core)].astype(BF16)
        dcopy(i).start()
    panels(14, 16)
    solver = lax.rem(col + zhi, 2) == core
    chip = zhi * 4 + col
    mine = 2 * col + zhi

    def rcopy(i):
        dev = {"row": 2 * lax.rem(core + i, 2) + core, "col": i}
        return remote(r2.at[i], r2in.at[chip], rsems.at[i], rrecv.at[chip], dev)

    def unless_mine(d, action):
        if d:
            action()
        else:
            pl.when(jnp.logical_not(solver))(action)

    for d in (2, 1, 3, 0):
        i = lax.rem(col + d, 4)
        arrived(rin.at[i], drecv.at[i])
        r2[i] = (rp[group(i, core)] + rin[i].astype(F32)).astype(BF16)
        unless_mine(d, lambda i=i: rcopy(i).start())
    for b in range(1, 4):
        flip(lax.rem(x + b, 4))

    def zforward(d):
        q = group(lax.rem(col + d, 4), core)
        return remote(zb.at[q], zb.at[q], zfwd.at[d], zrecv.at[q], partner)

    def zcopy(e):
        dev = {
            "row": 2 * lax.rem(zhi + e // 4, 2) + core, "col": lax.rem(col + e % 4, 4)
        }
        return remote(zb.at[mine], zb.at[mine], zsend.at[e], zrecv.at[mine], dev)

    @pl.when(solver)
    def _():
        whole = rp[mine] + rin[col].astype(F32)
        for e in range(1, 8):
            other = lax.rem(chip + e, 8)
            arrived(r2in.at[other], rrecv.at[other])
            whole = whole + r2in[other].astype(F32)
        zb[mine] = whole.astype(BF16)
        for e in (6, 5, 7, 4, 2, 1, 3):
            zcopy(e).start()
        zforward(0).start()

    inverse = jnp.concatenate([big[2], big[3]], axis=1)
    both_sides = lax.dot_general(
        inverse, inverse, (((0,), (0,)), ((), ())), precision=HIGHEST,
        preferred_element_type=F32,
    )
    sh, sl, _ = split3(both_sides)
    halves = jnp.concatenate([sh, sl], axis=1)
    for k in range(7):
        rows = slice(256 * k, 256 * k + 256)
        pair = jnp.dot(sm[rows, :], halves, preferred_element_type=F32)
        sm[rows, :] = (pair[:, :PANEL] + pair[:, PANEL:]).astype(BF16)

    def pass_answer(d):
        q = group(lax.rem(col + d, 4), core)

        def pass_on_sum():
            arrived(zb.at[q], zrecv.at[q])
            zforward(d).start()

        unless_mine(d, pass_on_sum)

    def correct(d):
        i = lax.rem(col + d, 4)
        q = group(i, 1 - core)
        arrived(zb.at[q], zrecv.at[q])
        both = jnp.concatenate([zb[2 * i], zb[2 * i + 1]], axis=1)
        lanes = pl.ds(pl.multiple_of(256 * i, 256), 256)
        corout[:, lanes] = jnp.dot(
            sm[...], both, preferred_element_type=F32
        ).astype(BF16)

    pass_answer(1)
    pass_answer(3)
    pass_answer(0)
    correct(0)
    pass_answer(2)
    these = pl.ds(pl.multiple_of(64 * row, 64), 64)
    right_side = jnp.concatenate([zb[2 * col], zb[2 * col + 1]], axis=1)
    solout[...] = jnp.dot(
        jnp.concatenate([big[2, these, :], big[3, these, :]], axis=1),
        right_side.astype(F32), precision=HIGHEST, preferred_element_type=F32,
    )
    correct(1)
    correct(3)
    correct(2)

    @pl.when(source)
    def _():
        for k in range(2):
            for dz in range(2):
                for e in range(16):
                    if dz or e:
                        scatter(k, dz, e).wait_send()

    for d in range(7):
        for slot in range(4):
            when_there(
                at(*offsets[d]), slot, lambda slot=slot: xcopy(d, slot).wait_send()
            )
    for k in range(2):
        for d in range(4):
            across(k, d).wait_send()
            if d:
                spread(k, d).wait_send()
                for b in range(4):
                    along(k, b, d).wait_send()
    for slot in range(4):
        def sent(slot=slot):
            for copy in own_sends(slot):
                copy.wait_send()
            for copy in relay_z(slot):
                copy.wait_send()
            relay_far(slot).wait_send()

        when_there(t, slot, sent)
        when_there(
            left if slot < 2 else right, slot,
            lambda slot=slot: relay_x(slot)[1].wait_send(),
        )

    for d in range(4):
        dcopy(d).wait_send()
        zforward(d).wait_send()
        unless_mine(d, lambda: rcopy(lax.rem(col + d, 4)).wait_send())

    @pl.when(solver)
    def _():
        for e in range(1, 8):
            zcopy(e).wait_send()


def body(activations, weights):
    dma = pltpu.SemaphoreType.DMA
    vmem = pltpu.VMEM
    outs = pl.pallas_call(
        kernel,
        out_shape=(
            jax.ShapeDtypeStruct((1792, 1024), BF16),
            jax.ShapeDtypeStruct((64, 256), F32),
        ),
        in_specs=[pl.BlockSpec(memory_space=pltpu.HBM)] * 2,
        out_specs=(pl.BlockSpec(memory_space=pltpu.VMEM),) * 2,
        scratch_shapes=[
            vmem((2, 128, 1792), BF16), vmem((3712, 1024), BF16),
            vmem((2, 2, 16, 256), BF16), vmem((2, 2, 4, 2, 4, 16, 256), BF16),
            vmem((256, 1024), BF16),
            vmem((4, 8, 128, 128), BF16), vmem((8, 4, 256, 128), BF16),
            vmem((8, 256, 128), F32), vmem((4, 256, 128), BF16),
            vmem((4, 256, 128), BF16), vmem((4, 256, 128), BF16),
            vmem((8, 256, 128), BF16), vmem((8, 256, 128), BF16),
            vmem((4, 256, 128), F32), vmem((1792, 256), BF16),
            dma, dma((2,)), dma((2, 2, 16)), dma((2, 2)), dma((8,)), dma((2, 4)), dma((32,)),
            dma((2, 4)), dma((8,)), dma((2,)), dma((32,)), dma((4,)), dma((12,)), dma((8, 4)),
            dma((16,)), dma((4,)), dma((4,)), dma((4,)),
            dma((8,)), dma((8,)), dma((4,)), dma((8,)),
        ],
        compiler_params=pltpu.CompilerParams(
            collective_id=0, has_side_effects=True, vmem_limit_bytes=48_000_000
        ),
    )(pltpu.with_memory_space_constraint(activations, pltpu.HBM), weights)
    correction, solved = outs
    return solved, correction


def solution(mesh):
    in_specs = (P(None, "tok", ("row", "col")), P(None, ("row", "col"), "tok"))
    out_specs = (P("row", ("tok", "col")), P(("row", "col"), "tok"))
    return jax.shard_map(
        body, mesh=mesh, in_specs=in_specs, out_specs=out_specs, check_vma=False
    )
```
